128 devices in a mesh: gx: 4 (over z), gy: 16 (over y, x), gz: 2 (over core).
Axes of the slice: x: 4, y: 4, z: 4, core: 2. Of those that a mesh axis runs over, the one named last changes fastest.
Arguments:
- particles: float32 [8, 1048576], P(None, ('gx', 'gy', 'gz')), may hold values from -0.5 to 0.5
- dest_key: int32 [1048576], P(('gx', 'gy', 'gz')), may hold values from 0 to 127, as said below
- cell_a: int32 [1048576], P(('gx', 'gy', 'gz')), may hold values from 0 to 255
- cell_b: int32 [1048576], P(('gx', 'gy', 'gz')), may hold values from 0 to 127
- velocity: float32 [2, 1024, 4096], P(None, 'gx', ('gy', 'gz')), may hold values from -6 to 6
Outputs:
- binned: float32 [8, 4194304], P(None, ('gx', 'gy', 'gz'))
- binned_cell: int32 [4194304], P(('gx', 'gy', 'gz'))
The draws below stay inside these ranges and needn't reach their ends.
Inputs may be any that keep to these rules, and one draw needn't show every extreme that they name: Of the particles of one device at most 256 have any one value of dest_key, and one device is named by exactly 256 particles of every device.
All inputs are finite; a program needn't handle non-finite values.
Results may differ from the reference program's by a relative error of at most 0.0003.
Values sent between devices are 32-bit elements; how exact they have to be, the bound alone decides.
A program may use at most 64 MiB of HBM per device.

```python
import jax
import jax.numpy as jnp
from jax import lax

P_DEV = 8192
TA = 256
TB = 128
OWNERS = 128
CAP = 256
TOTAL = 1048576
NA = 1024
NB = 4096
N_GY = 16
N_GZ = 2


def draw_dest_key(key, part):
    hot_owner = jax.random.randint(jax.random.fold_in(key, 7), (), 0, OWNERS)
    slot_owner = (jnp.arange(OWNERS * CAP, dtype=jnp.int32) // CAP + hot_owner) % OWNERS

    def one_source(source_dev):
        source_key = jax.random.fold_in(key, source_dev)
        others = jax.random.permutation(source_key, OWNERS * CAP - CAP).astype(jnp.int32) + CAP
        chosen = jnp.concatenate([jnp.arange(CAP, dtype=jnp.int32), others[:P_DEV - CAP]])
        shuffle = jax.random.permutation(jax.random.fold_in(source_key, 1), P_DEV)
        return slot_owner[chosen][shuffle]
    return lax.map(one_source, jnp.arange(OWNERS, dtype=jnp.int32)).reshape(-1)


def place_ends(array, stream_key, smallest, top_value):
    longest = array.shape.index(max(array.shape))
    spots = []
    for shift in (0, 1):
        where = [jax.random.randint(jax.random.fold_in(stream_key, axis), (), 0, length) for axis, length in enumerate(array.shape)]
        where[longest] = (where[longest] + shift) % array.shape[longest]
        spots.append(tuple(where))
    return array.at[spots[0]].set(smallest).at[spots[1]].set(top_value)


def level_of(rng, extent, split, low, high):
    def one(dim, shards_of):
        heights = jax.random.uniform(jax.random.fold_in(jax.random.fold_in(rng, 6), dim), (shards_of,), jnp.float32, low / len(split), high / len(split))
        return jnp.repeat(jnp.exp(heights), extent[dim] // shards_of).reshape((-1,) + (1,) * (len(extent) - dim - 1))

    gain = one(*split[0])
    for cut in split[1:]:
        gain = gain * one(*cut)
    return gain


def scatter_about(key, shape, spread, limit, cuts=(), held_as=jnp.bfloat16):
    drawn = spread * jax.random.normal(key, shape, jnp.float32)
    if cuts:
        drawn = drawn * level_of(key, shape, cuts, -0.22, 0.18)
    return jnp.clip(drawn, -limit, limit).astype(held_as)


def setup_inputs(seed: int = 0) -> dict:
    splits = jax.random.split(jax.random.key(seed), 6)
    particles = jnp.clip(jax.random.uniform(splits[0], (8, TOTAL), jnp.float32, -0.5, 0.5) * level_of(splits[0], (8, TOTAL), ((1, 128),), -0.4, 0.0), -0.5, 0.5)
    dest_key = draw_dest_key(jax.random.fold_in(splits[5], 71), 0)
    cell_a = place_ends(jax.random.randint(splits[2], (TOTAL,), 0, TA), jax.random.fold_in(splits[2], 1), 0, TA - 1).astype(jnp.int32)
    cell_b = place_ends(jax.random.randint(splits[3], (TOTAL,), 0, TB), jax.random.fold_in(splits[3], 1), 0, TB - 1).astype(jnp.int32)
    velocity = scatter_about(splits[4], (2, NA, NB), 1.0, 6.0, ((1, 4), (2, 32)), jnp.float32)
    return {"particles": particles, "dest_key": dest_key, "cell_a": cell_a, "cell_b": cell_b, "velocity": velocity}


step_length = 0.5


def quad_weights(frac):
    return (0.5 * frac * (frac - 1.0), 1.0 - frac * frac, 0.5 * frac * (frac + 1.0))


def reference(particles, dest_key, cell_a, cell_b, velocity):
    source_dev = jnp.arange(TOTAL, dtype=jnp.int32) // P_DEV
    bucket_key = source_dev * OWNERS + dest_key
    ordering = jnp.argsort(bucket_key, stable=True).astype(jnp.int32)
    ordered = bucket_key[ordering]
    first_index = jnp.searchsorted(ordered, ordered, side="left").astype(jnp.int32)
    rank_sorted = jnp.arange(TOTAL, dtype=jnp.int32) - first_index
    ranking = jnp.zeros((TOTAL,), jnp.int32).at[ordering].set(rank_sorted)
    slot_index = dest_key * (OWNERS * CAP) + source_dev * CAP + ranking
    tile_columns = N_GY * N_GZ
    global_a = (dest_key // tile_columns) * TA + cell_a
    global_b = (dest_key % tile_columns) * TB + cell_b
    padded = jnp.pad(velocity, ((0, 0), (1, 1), (1, 1)))
    row_stride = NB + 2
    flat_field = padded.reshape(2, -1)
    center = ((global_a + 1) * row_stride + global_b + 1).astype(jnp.int32)
    weights_a = quad_weights(particles[0])
    weights_b = quad_weights(particles[1])
    speed = jnp.zeros((2, TOTAL), jnp.float32)
    for shift_a in range(3):
        for shift_b in range(3):
            nodes = flat_field[:, center + (shift_a - 1) * row_stride + (shift_b - 1)]
            speed = speed + weights_a[shift_a] * weights_b[shift_b] * nodes
    advanced = jnp.concatenate([particles[0:2], particles[2:4] + step_length * speed, particles[4:8]], axis=0)
    binned = jnp.zeros((8, OWNERS * OWNERS * CAP), particles.dtype).at[:, slot_index].set(advanced)
    binned_cell = jnp.full((OWNERS * OWNERS * CAP,), -1, jnp.int32).at[slot_index].set(cell_a * TB + cell_b)
    return binned, binned_cell
```

```python
import functools

import jax
import jax.numpy as jnp
from jax import lax
from jax.experimental import pallas as pl
from jax.experimental.pallas import tpu as pltpu
from jax.sharding import PartitionSpec as P

step_length = 0.5
NT = (((1,), (1,)), ((), ()))
LANES = 128
BLOCK_A, BLOCK_B = 4, 32
DIRS = ((-1, -1), (-1, 0), (-1, 1), (0, -1), (0, 1), (1, -1), (1, 0), (1, 1))


def quad_weights(frac):
    return (0.5 * frac * (frac - 1.0), 1.0 - frac * frac, 0.5 * frac * (frac + 1.0))


def rounded(x):
    return x.astype(jnp.bfloat16).astype(jnp.float32)


def narrow_iota(shape, dim):
    return lax.broadcasted_iota(jnp.int32, shape, dim).astype(jnp.float32).astype(jnp.bfloat16)


def one_hot(row, index):
    one, zero = jnp.ones((), jnp.bfloat16), jnp.zeros((), jnp.bfloat16)
    return jnp.where(row == index, one, zero)


def pack_edges(vel_ref, edge_ref):
    tile_height, tile_width = vel_ref.shape[1:]
    edge_ref[...] = jnp.zeros_like(edge_ref)
    for c in range(2):
        edge_ref[4 * c:4 * c + 1, :tile_width] = vel_ref[c, 0:1, :]
        edge_ref[4 * c + 1:4 * c + 2, :tile_width] = vel_ref[c, tile_height - 1:, :]
        turned = jnp.transpose(vel_ref[c])
        edge_ref[4 * c + 2:4 * c + 3, :tile_height] = turned[0:1]
        edge_ref[4 * c + 3:4 * c + 4, :tile_height] = turned[tile_width - 1:]


def sort_particles(owners, width, chunk, part_ref, key_ref, a_ref, b_ref,
                   hot_ref, base_ref, pick_ref, low_ref, acc_ref, sorted_ref, cells_ref, table_ref):
    count = key_ref.shape[1]
    owner_rows = narrow_iota((owners, width), 0)
    ones = jnp.ones((width, LANES), jnp.bfloat16)
    base_ref[...] = jnp.zeros_like(base_ref)
    tops = count // width

    def count_chunk(index, seen):
        for part in range(chunk // width):
            start = pl.multiple_of(index * chunk + part * width, width)
            keys = key_ref[:, pl.ds(start, width)].astype(jnp.float32).astype(jnp.bfloat16)
            hot = one_hot(owner_rows, keys)
            hot_ref[:, pl.ds(start, width)] = hot
            base_ref[index * (chunk // width) + part] = seen
            seen = seen + jnp.dot(hot, ones, preferred_element_type=jnp.float32)
        return seen

    total = lax.fori_loop(0, count // chunk, count_chunk, jnp.zeros((owners, LANES), jnp.float32))
    below = (lax.broadcasted_iota(jnp.int32, (owners, owners), 1)
             < lax.broadcasted_iota(jnp.int32, (owners, owners), 0)).astype(jnp.float32).astype(jnp.bfloat16)
    first = jnp.dot(below, total.astype(jnp.bfloat16), preferred_element_type=jnp.float32)
    eye = (lax.broadcasted_iota(jnp.int32, (owners, LANES), 1)
           == lax.broadcasted_iota(jnp.int32, (owners, LANES), 0))
    firsts = jnp.sum(jnp.where(eye, first, 0.0), axis=0, keepdims=True)
    totals = jnp.sum(jnp.where(eye, total, 0.0), axis=0, keepdims=True)
    table_ref[0:1, :] = firsts.astype(jnp.int32)
    table_ref[1:2, :] = totals.astype(jnp.int32)

    upper = (lax.broadcasted_iota(jnp.int32, (width, width), 0)
             < lax.broadcasted_iota(jnp.int32, (width, width), 1)).astype(jnp.float32).astype(jnp.bfloat16)
    owner_ids = lax.broadcasted_iota(jnp.int32, (owners, LANES), 0)
    low_rows = narrow_iota((width, width), 0)
    top_rows = narrow_iota((tops, width), 0)
    zero = jnp.zeros((), jnp.bfloat16)

    acc_ref[...] = jnp.zeros_like(acc_ref)

    def place_chunk(index, carry):
        for part in range(chunk // width):
            start = pl.multiple_of(index * chunk + part * width, width)
            at = slice(part * width, (part + 1) * width)
            before = jnp.dot(hot_ref[:, pl.ds(start, width)], upper, preferred_element_type=jnp.float32)
            base = base_ref[index * (chunk // width) + part] + first
            keys = key_ref[:, pl.ds(start, width)]
            spots = []
            for j in range(width // LANES):
                cut = slice(j * LANES, (j + 1) * LANES)
                spots.append(jnp.sum(jnp.where(owner_ids == keys[:, cut], before[:, cut] + base, 0.0),
                                     axis=0, keepdims=True))
            spot = jnp.concatenate(spots, axis=1).astype(jnp.int32)
            top_int = spot // width
            top = top_int.astype(jnp.float32).astype(jnp.bfloat16)
            low = (spot - top_int * width).astype(jnp.float32).astype(jnp.bfloat16)
            low_ref[:, at] = one_hot(low_rows, low)
            values = part_ref[:, pl.ds(start, width)]
            high = rounded(values)
            both = jnp.concatenate([high, values - high], axis=0).astype(jnp.bfloat16)
            for i in range(tops):
                pick_ref[i * 16:(i + 1) * 16, at] = jnp.where(top == jnp.full((), i, jnp.bfloat16), both, zero)
            rows = a_ref[:, pl.ds(start, width)].astype(jnp.float32).astype(jnp.bfloat16)
            cols = b_ref[:, pl.ds(start, width)].astype(jnp.float32).astype(jnp.bfloat16)
            mine = top_rows == top
            pick_ref[tops * 16:tops * 17, at] = jnp.where(mine, rows, zero)
            pick_ref[tops * 17:tops * 18, at] = jnp.where(mine, cols, zero)
        acc_ref[...] += lax.dot_general(pick_ref[...], low_ref[...], NT, preferred_element_type=jnp.float32)
        return carry

    lax.fori_loop(0, count // chunk, place_chunk, 0)


def unpack_sorted(tops, width, tile_width, acc_ref, sorted_ref, cells_ref):
    cells = acc_ref[tops * 16:tops * 17, :] * float(tile_width) + acc_ref[tops * 17:tops * 18, :]
    for i in range(tops):
        at = slice(i * width, (i + 1) * width)
        sorted_ref[:, at] = acc_ref[i * 16:i * 16 + 8, :] + acc_ref[i * 16 + 8:i * 16 + 16, :]
        cells_ref[0:1, at] = cells[i:i + 1, :]


def cut_block(first, size, sorted_ref, cells_ref, out):
    base = pl.multiple_of((first // LANES) * LANES, LANES)
    shift = first - base
    back = lax.rem(LANES - shift, LANES)
    lane = lax.broadcasted_iota(jnp.int32, (8, LANES), 1)
    near = lane < LANES - shift
    for source, rows in ((sorted_ref, 8), (cells_ref, 1)):
        turned = [pltpu.roll(source[:, pl.ds(base + j * LANES, LANES)], back, 1) for j in range(3)]
        for j in range(2):
            piece = jnp.where(near, turned[j], turned[j + 1])
            if rows == 8:
                out[8 * j:8 * j + 8, :] = jnp.where(lane + j * LANES < size, piece, 0.0)
            else:
                out[16 + j:17 + j, :] = jnp.where(lane + j * LANES < size, piece, -1.0)[0:1]


def build_table(vel_ref, halo_ref, table_ref, tile_height, tile_width):
    width = tile_width + 8
    lane = lax.broadcasted_iota(jnp.int32, (1, LANES), 1)
    tall = tile_height // BLOCK_A
    wide = tile_width // BLOCK_B
    reach = BLOCK_A + 2
    node = lax.broadcasted_iota(jnp.int32, (tile_height + LANES, reach * tall), 0)
    slot = lax.broadcasted_iota(jnp.int32, (tile_height + LANES, reach * tall), 1)
    want = BLOCK_A * (slot % tall) + slot // tall - 1
    want = jnp.where(want < 0, tile_height, jnp.where(want == tile_height, tile_height + 1, want))
    select = (node == want).astype(jnp.float32).astype(jnp.bfloat16)

    def beside(da, db, row):
        return halo_ref[DIRS.index((da, db)), row:row + 1, :]

    for c in range(2):
        own = jnp.transpose(vel_ref[c])
        left = beside(0, -1, 4 * c + 3)[:, :tile_height]
        right = beside(0, 1, 4 * c + 2)[:, :tile_height]
        rest = jnp.zeros((width - tile_width - 2, tile_height), jnp.float32)
        body = jnp.concatenate([own, left, right, rest], axis=0)

        def outer(da, row):
            middle = beside(da, 0, row)[:, :tile_width]
            west = beside(da, -1, row)[:, tile_width - 1:tile_width]
            east = beside(da, 1, row)[:, 0:1]
            return jnp.concatenate(
                [middle, jnp.where(lane == 0, west, jnp.where(lane == 1, east, 0.0))], axis=1)

        ends = jnp.concatenate([outer(-1, 4 * c + 1), outer(1, 4 * c),
                                jnp.zeros((LANES - 2, 2 * LANES), jnp.float32)], axis=0)
        full = jnp.concatenate([body, jnp.transpose(ends)[:width]], axis=1)
        high = rounded(full)
        both = jnp.concatenate([high, full - high], axis=0).astype(jnp.bfloat16)
        spread = jnp.dot(both, select, preferred_element_type=jnp.float32)
        first_half = lax.broadcasted_iota(jnp.int32, (BLOCK_B, LANES), 1) < LANES // 2
        for part in range(2):
            z = spread[part * width:(part + 1) * width]
            plain = [z[:, j * LANES:(j + 1) * LANES] for j in range(reach * tall // LANES)]
            turned = [pltpu.roll(p, LANES // 2, 1) for p in plain]

            def joined(i, rows):
                j, half = i // 2, i % 2
                low, top = (plain[j], turned[j]) if half == 0 else (turned[j], plain[j])
                height = rows[0].stop - rows[0].start
                return jnp.concatenate([jnp.where(first_half[:height], low[rows[2 * k]], top[rows[2 * k + 1]])
                                        for k in range(wide // 2)], axis=1)

            columns = slice(part * tall * wide, (part + 1) * tall * wide)
            for i in range(reach):
                low = (c * reach + i) * BLOCK_B
                table_ref[low:low + BLOCK_B, columns] = joined(
                    i, [slice(BLOCK_B * k, BLOCK_B * (k + 1)) for k in range(wide)]).astype(jnp.bfloat16)
            for e in range(2):
                if e == 0:
                    lines = [tile_width] + [BLOCK_B * k - 1 for k in range(1, wide)]
                else:
                    lines = [BLOCK_B * (k + 1) for k in range(wide - 1)] + [tile_width + 1]
                rows = [joined(i, [slice(r, r + 1) for r in lines]) for i in range(reach)]
                rows.append(jnp.zeros((8 - reach, tall * wide), jnp.float32))
                low = 2 * reach * BLOCK_B + (c * 2 + e) * 8
                table_ref[low:low + 8, columns] = jnp.concatenate(rows, axis=0).astype(jnp.bfloat16)


def gather_nodes(blocks, tile_width, table_ref, nodes_ref):
    cells = jnp.concatenate([b[16 + j:17 + j, :] for b in blocks for j in range(2)], axis=1)
    cell = jnp.maximum(cells, 0.0).astype(jnp.int32)
    row = cell // tile_width
    col = cell - row * tile_width
    index = (col // BLOCK_B) * 64 + row // BLOCK_A
    index = index.astype(jnp.float32).astype(jnp.bfloat16)
    hot = one_hot(narrow_iota((256, index.shape[1]), 0), index)
    nodes_ref[...] = jnp.dot(table_ref[...], jnp.concatenate([hot, hot], axis=0),
                             preferred_element_type=jnp.float32)


def banded(diff, weights):
    return jnp.where(diff == -1, weights[0], jnp.where(diff == 0, weights[1], jnp.where(diff == 1, weights[2], 0.0)))


def weigh(v, cell, tile_width, nodes, weights_ref):
    reach = BLOCK_A + 2
    live = cell >= 0.0
    place = jnp.maximum(cell, 0.0).astype(jnp.int32)
    row = place // tile_width
    col = place - row * tile_width
    row = row % BLOCK_A
    col = col % BLOCK_B
    wa = quad_weights(v[0:1])
    wb = quad_weights(v[1:2])
    aw = banded(lax.broadcasted_iota(jnp.int32, (8, LANES), 0) - 1 - row, wa)
    bw = banded(lax.broadcasted_iota(jnp.int32, (BLOCK_B, LANES), 0) - col, wb)
    left = jnp.where(col == 0, wb[0], 0.0)
    right = jnp.where(col == BLOCK_B - 1, wb[2], 0.0)
    scale = jnp.where(live, step_length, 0.0)
    moved = []
    for c in range(2):
        y = None
        for i in range(reach):
            term = aw[i:i + 1] * nodes(slice((c * reach + i) * BLOCK_B, (c * reach + i + 1) * BLOCK_B))
            y = term if y is None else y + term
        y = y * bw
        low = 2 * reach * BLOCK_B + c * 16
        z = aw * (left * nodes(slice(low, low + 8)) + right * nodes(slice(low + 8, low + 16)))
        for k in range(BLOCK_B // 8):
            z = z + y[8 * k:8 * k + 8]
        moved.append(jnp.sum(z, axis=0, keepdims=True) * scale)
    line = lax.broadcasted_iota(jnp.int32, v.shape, 0)
    return v + jnp.where(line == 2, moved[0], jnp.where(line == 3, moved[1], 0.0))


def advance_block(block, source, at, tile_width, nodes_ref, out_ref, cell_ref):
    for j in range(2):
        lanes = slice(at + j * LANES, at + (j + 1) * LANES)
        v = block[8 * j:8 * j + 8, :]
        cell = block[16 + j:17 + j, :]
        out_ref[:, pl.ds(pl.multiple_of(source * 2 * LANES + j * LANES, LANES), LANES)] = weigh(
            v, cell, tile_width, lambda rows, lanes=lanes: nodes_ref[rows, lanes], None)
    cell_ref[pl.ds(source * 2, 2), :] = block[16:18, :].astype(jnp.int32)


def sort_kernel(width, chunk, tile_width, part_ref, key_ref, a_ref, b_ref, blocks_ref,
                hot_ref, base_ref, pick_ref, low_ref, acc_ref, sorted_ref, cells_ref, first_ref, first_smem, local_sem):
    first_ref[...] = jnp.zeros_like(first_ref)
    sort_particles(blocks_ref.shape[0], width, chunk, part_ref, key_ref, a_ref, b_ref, hot_ref, base_ref, pick_ref,
                   low_ref, acc_ref, sorted_ref, cells_ref, first_ref)
    to_smem = pltpu.make_async_copy(first_ref, first_smem, local_sem)
    to_smem.start()
    tops = key_ref.shape[1] // width
    tail = tops * width
    sorted_ref[:, tail:] = jnp.zeros((8, sorted_ref.shape[1] - tail), jnp.float32)
    cells_ref[:, tail:] = jnp.zeros((8, cells_ref.shape[1] - tail), jnp.float32)
    unpack_sorted(tops, width, tile_width, acc_ref, sorted_ref, cells_ref)
    to_smem.wait()

    def cut(owner, carry):
        cut_block(first_smem[0, owner], first_smem[1, owner], sorted_ref, cells_ref, blocks_ref.at[owner])
        return carry

    lax.fori_loop(0, blocks_ref.shape[0], cut, 0, unroll=4)


def exchange_kernel(sizes, blocks_ref, vel_ref, out_ref, cell_ref, held, edge_ref, halo_ref, table_ref,
                    nodes_even, nodes_odd, send_sem, recv_sem, halo_send, halo_recv):
    nx, ny, nz = sizes
    plane = ny * nz
    n = nx * plane
    tile_height, tile_width = vel_ref.shape[1:]
    gx, gy, gz = lax.axis_index("gx"), lax.axis_index("gy"), lax.axis_index("gz")
    column = gy * nz + gz

    def at(dx, dyz, sign):
        x = lax.rem(gx + sign * dx + nx, nx)
        y = lax.rem(gy + sign * (dyz // nz) + ny, ny)
        z = lax.rem(gz + sign * lax.rem(dyz, nz) + nz, nz)
        return x, y, z

    def linear(place):
        return (place[0] * ny + place[1]) * nz + place[2]

    def halo_copy(k, slot):
        da, db = DIRS[k]
        there = column + db
        return pltpu.make_async_remote_copy(
            src_ref=edge_ref, dst_ref=halo_ref.at[slot], send_sem=halo_send.at[k],
            recv_sem=halo_recv.at[slot], device_id=(gx + da, there // nz, lax.rem(there, nz)),
            device_id_type=pl.DeviceIdType.MESH)

    def exists(k):
        da, db = DIRS[k]
        a, b = gx + da, column + db
        return (a >= 0) & (a < nx) & (b >= 0) & (b < plane)

    def hop(q):
        return lax.rem(q, nx), q // nx

    def block_copy(q):
        there = at(*hop(q), 1)
        return pltpu.make_async_remote_copy(
            src_ref=blocks_ref.at[linear(there)], dst_ref=held.at[q],
            send_sem=send_sem.at[q], recv_sem=recv_sem.at[q], device_id=there,
            device_id_type=pl.DeviceIdType.MESH)

    pack_edges(vel_ref, edge_ref)
    for k in range(8):
        @pl.when(exists(k))
        def _(k=k):
            halo_copy(k, 7 - k).start()

        @pl.when(jnp.logical_not(exists(k)))
        def _(k=k):
            halo_ref[k] = jnp.zeros(halo_ref.shape[1:], jnp.float32)

    def dispatch(q, carry):
        block_copy(q).start()
        return carry

    lax.fori_loop(1, n, dispatch, 0)
    held[0] = blocks_ref[linear((gx, gy, gz))]

    for k in range(8):
        @pl.when(exists(k))
        def _(k=k):
            halo_copy(k, k).wait_recv()

    build_table(vel_ref, halo_ref, table_ref, tile_height, tile_width)

    def gather(t, nodes_ref):
        gather_nodes([held.at[2 * t], held.at[2 * t + 1]], tile_width, table_ref, nodes_ref)

    def weigh_pair(t, nodes_ref):
        for i in range(2):
            source = linear(at(*hop(2 * t + i), -1))
            advance_block(held.at[2 * t + i], source, i * 2 * LANES, tile_width, nodes_ref, out_ref, cell_ref)

    block_copy(1).wait_recv()
    gather(0, nodes_even)

    def both(t, carry):
        block_copy(4 * t + 2).wait_recv()
        block_copy(4 * t + 3).wait_recv()
        gather(2 * t + 1, nodes_odd)
        weigh_pair(2 * t, nodes_even)

        @pl.when(t + 1 < n // 4)
        def _():
            block_copy(4 * t + 4).wait_recv()
            block_copy(4 * t + 5).wait_recv()

        gather(jnp.minimum(2 * t + 2, n // 2 - 1), nodes_even)
        weigh_pair(2 * t + 1, nodes_odd)
        return carry

    lax.fori_loop(0, n // 4, both, 0)

    def sent(q, carry):
        block_copy(q).wait_send()
        return carry

    lax.fori_loop(1, n, sent, 0)
    for k in range(8):
        @pl.when(exists(k))
        def _(k=k):
            halo_copy(k, 7 - k).wait_send()


def shards(particles, dest_key, cell_a, cell_b, velocity):
    owners = lax.axis_size(("gx", "gy", "gz"))
    count = particles.shape[1]
    cap = 4 * count // owners
    tile_height, tile_width = velocity.shape[1:]
    assert owners == LANES and cap == 2 * LANES and (tile_height, tile_width) == (256, 128)
    width, chunk = 256, 1024
    tops = count // width
    sizes = tuple(lax.axis_size(name) for name in ("gx", "gy", "gz"))
    in_vmem = pl.BlockSpec(memory_space=pltpu.VMEM)
    blocks = pl.pallas_call(
        functools.partial(sort_kernel, width, chunk, tile_width),
        out_shape=jax.ShapeDtypeStruct((owners, 18, LANES), jnp.float32),
        in_specs=[in_vmem] * 4,
        out_specs=in_vmem,
        scratch_shapes=[
            pltpu.VMEM((owners, count), jnp.bfloat16),
            pltpu.VMEM((tops, owners, LANES), jnp.float32),
            pltpu.VMEM((tops * 18, chunk), jnp.bfloat16),
            pltpu.VMEM((width, chunk), jnp.bfloat16),
            pltpu.VMEM((tops * 18, width), jnp.float32),
            pltpu.VMEM((8, count + 3 * LANES), jnp.float32),
            pltpu.VMEM((8, count + 3 * LANES), jnp.float32),
            pltpu.VMEM((8, LANES), jnp.int32),
            pltpu.SMEM((8, LANES), jnp.int32),
            pltpu.SemaphoreType.DMA,
        ],
    )(particles, dest_key.reshape(1, -1), cell_a.reshape(1, -1), cell_b.reshape(1, -1))
    rows = 12 * BLOCK_B + 32
    binned, binned_cell = pl.pallas_call(
        functools.partial(exchange_kernel, sizes),
        out_shape=(jax.ShapeDtypeStruct((8, owners * cap), jnp.float32),
                   jax.ShapeDtypeStruct((owners * 2, LANES), jnp.int32)),
        in_specs=[in_vmem] * 2,
        out_specs=(in_vmem,) * 2,
        scratch_shapes=[
            pltpu.VMEM((owners, 18, LANES), jnp.float32),
            pltpu.VMEM((8, max(tile_height, tile_width)), jnp.float32),
            pltpu.VMEM((8, 8, max(tile_height, tile_width)), jnp.float32),
            pltpu.VMEM((rows, 2 * 256), jnp.bfloat16),
            pltpu.VMEM((rows, 4 * LANES), jnp.float32),
            pltpu.VMEM((rows, 4 * LANES), jnp.float32),
            pltpu.SemaphoreType.DMA((owners,)),
            pltpu.SemaphoreType.DMA((owners,)),
            pltpu.SemaphoreType.DMA((8,)),
            pltpu.SemaphoreType.DMA((8,)),
        ],
        compiler_params=pltpu.CompilerParams(has_side_effects=True),
    )(blocks, velocity)
    return (binned, binned_cell.reshape(-1))


def solution(mesh):
    in_specs = (
        P(None, ("gx", "gy", "gz")),
        P(("gx", "gy", "gz")),
        P(("gx", "gy", "gz")),
        P(("gx", "gy", "gz")),
        P(None, "gx", ("gy", "gz")),
    )
    out_specs = (P(None, ("gx", "gy", "gz")), P(("gx", "gy", "gz")))
    return jax.shard_map(shards, mesh=mesh, in_specs=in_specs, out_specs=out_specs, check_vma=False)
```

```python
import functools

import jax
import jax.numpy as jnp
from jax import lax
from jax.experimental import pallas as pl
from jax.experimental.pallas import tpu as pltpu
from jax.sharding import PartitionSpec as P

step_length = 0.5
NT = (((1,), (1,)), ((), ()))
LANES = 128
BLOCK_A, BLOCK_B = 4, 32
DIRS = ((-1, -1), (-1, 0), (-1, 1), (0, -1), (0, 1), (1, -1), (1, 0), (1, 1))


def quad_weights(frac):
    return (0.5 * frac * (frac - 1.0), 1.0 - frac * frac, 0.5 * frac * (frac + 1.0))


def rounded(x):
    return x.astype(jnp.bfloat16).astype(jnp.float32)


def narrow_iota(shape, dim):
    return lax.broadcasted_iota(jnp.int32, shape, dim).astype(jnp.float32).astype(jnp.bfloat16)


def one_hot(row, index):
    one, zero = jnp.ones((), jnp.bfloat16), jnp.zeros((), jnp.bfloat16)
    return jnp.where(row == index, one, zero)


def pack_edges(vel_ref, edge_ref):
    tile_height, tile_width = vel_ref.shape[1:]
    edge_ref[...] = jnp.zeros_like(edge_ref)
    for c in range(2):
        edge_ref[4 * c:4 * c + 1, :tile_width] = vel_ref[c, 0:1, :]
        edge_ref[4 * c + 1:4 * c + 2, :tile_width] = vel_ref[c, tile_height - 1:, :]
        turned = jnp.transpose(vel_ref[c])
        edge_ref[4 * c + 2:4 * c + 3, :tile_height] = turned[0:1]
        edge_ref[4 * c + 3:4 * c + 4, :tile_height] = turned[tile_width - 1:]


def sort_particles(owners, width, chunk, part_ref, key_ref, a_ref, b_ref,
                   hot_ref, base_ref, pick_ref, low_ref, acc_ref, sorted_ref, cells_ref, table_ref):
    count = key_ref.shape[1]
    owner_rows = narrow_iota((owners, width), 0)
    ones = jnp.ones((width, LANES), jnp.bfloat16)
    owner_ids = lax.broadcasted_iota(jnp.int32, (owners, LANES), 0)
    tops = count // width

    def count_chunk(index, carry):
        seen, tally = carry
        for part in range(chunk // width):
            start = pl.multiple_of(index * chunk + part * width, width)
            keys = key_ref[:, pl.ds(start, width)]
            hot = one_hot(owner_rows, keys.astype(jnp.float32).astype(jnp.bfloat16))
            hot_ref[:, pl.ds(start, width)] = hot
            base_ref[index * (chunk // width) + part] = seen
            seen = seen + jnp.dot(hot, ones, preferred_element_type=jnp.float32)
            for j in range(width // LANES):
                tally = tally + jnp.where(owner_ids == keys[:, j * LANES:(j + 1) * LANES], 1, 0)
        return seen, tally

    total, tally = lax.fori_loop(0, count // chunk, count_chunk, (
        jnp.zeros((owners, LANES), jnp.float32), jnp.zeros((owners, LANES), jnp.int32)))
    tally = jnp.sum(tally, axis=1, keepdims=True)
    below = (lax.broadcasted_iota(jnp.int32, (owners, owners), 1)
             < lax.broadcasted_iota(jnp.int32, (owners, owners), 0)).astype(jnp.float32).astype(jnp.bfloat16)
    first = jnp.dot(below, total.astype(jnp.bfloat16), preferred_element_type=jnp.float32)
    lane_ids = lax.broadcasted_iota(jnp.int32, (owners, LANES), 1)
    table_ref[0:1, :] = jnp.sum(jnp.where(owner_ids < lane_ids, tally, 0), axis=0, keepdims=True)
    table_ref[1:2, :] = jnp.sum(jnp.where(owner_ids == lane_ids, tally, 0), axis=0, keepdims=True)

    upper = (lax.broadcasted_iota(jnp.int32, (width, width), 0)
             < lax.broadcasted_iota(jnp.int32, (width, width), 1)).astype(jnp.float32).astype(jnp.bfloat16)
    low_rows = narrow_iota((width, width), 0)
    top_rows = narrow_iota((tops, width), 0)
    zero = jnp.zeros((), jnp.bfloat16)

    acc_ref[...] = jnp.zeros_like(acc_ref)

    def place_chunk(index, carry):
        for part in range(chunk // width):
            start = pl.multiple_of(index * chunk + part * width, width)
            at = slice(part * width, (part + 1) * width)
            before = jnp.dot(hot_ref[:, pl.ds(start, width)], upper, preferred_element_type=jnp.float32)
            base = base_ref[index * (chunk // width) + part] + first
            keys = key_ref[:, pl.ds(start, width)]
            spots = []
            for j in range(width // LANES):
                cut = slice(j * LANES, (j + 1) * LANES)
                spots.append(jnp.sum(jnp.where(owner_ids == keys[:, cut], before[:, cut] + base, 0.0),
                                     axis=0, keepdims=True))
            spot = jnp.concatenate(spots, axis=1).astype(jnp.int32)
            top_int = spot // width
            top = top_int.astype(jnp.float32).astype(jnp.bfloat16)
            low = (spot - top_int * width).astype(jnp.float32).astype(jnp.bfloat16)
            low_ref[:, at] = one_hot(low_rows, low)
            values = part_ref[:, pl.ds(start, width)]
            high = rounded(values)
            both = jnp.concatenate([high, values - high], axis=0).astype(jnp.bfloat16)
            for i in range(tops):
                pick_ref[i * 16:(i + 1) * 16, at] = jnp.where(top == jnp.full((), i, jnp.bfloat16), both, zero)
            rows = a_ref[:, pl.ds(start, width)].astype(jnp.float32).astype(jnp.bfloat16)
            cols = b_ref[:, pl.ds(start, width)].astype(jnp.float32).astype(jnp.bfloat16)
            mine = top_rows == top
            pick_ref[tops * 16:tops * 17, at] = jnp.where(mine, rows, zero)
            pick_ref[tops * 17:tops * 18, at] = jnp.where(mine, cols, zero)
        acc_ref[...] += lax.dot_general(pick_ref[...], low_ref[...], NT, preferred_element_type=jnp.float32)
        return carry

    lax.fori_loop(0, count // chunk, place_chunk, 0)


def unpack_sorted(tops, width, tile_width, acc_ref, sorted_ref, cells_ref):
    cells = acc_ref[tops * 16:tops * 17, :] * float(tile_width) + acc_ref[tops * 17:tops * 18, :]
    per = width // LANES
    for i in range(tops):
        rows = acc_ref[i * 16:i * 16 + 8, :] + acc_ref[i * 16 + 8:i * 16 + 16, :]
        for j in range(per):
            at = slice(j * LANES, (j + 1) * LANES)
            sorted_ref[i * per + j] = rows[:, at]
            cells_ref[i * per + j, 0:1] = cells[i:i + 1, at]


def cut_block(first, size, sorted_ref, cells_ref, out):
    base = first // LANES
    shift = first - base * LANES
    back = LANES - shift
    lane = lax.broadcasted_iota(jnp.int32, (8, LANES), 1)
    near = lane < back
    turned = [pltpu.roll(sorted_ref[base + j], back, 1) for j in range(3)]
    for j in range(2):
        piece = jnp.where(near, turned[j], turned[j + 1])
        out[8 * j:8 * j + 8, :] = jnp.where(lane + j * LANES < size, piece, 0.0)
    turned = [pltpu.roll(cells_ref[base + j], back, 1) for j in range(3)]
    for j in range(2):
        piece = jnp.where(near, turned[j], turned[j + 1])
        out[16 + j:17 + j, :] = jnp.where(lane + j * LANES < size, piece, -1.0)[0:1]


def build_table(vel_ref, halo_ref, table_ref, tile_height, tile_width):
    width = tile_width + 8
    lane = lax.broadcasted_iota(jnp.int32, (1, LANES), 1)
    tall = tile_height // BLOCK_A
    wide = tile_width // BLOCK_B
    reach = BLOCK_A + 2
    node = lax.broadcasted_iota(jnp.int32, (tile_height + LANES, reach * tall), 0)
    slot = lax.broadcasted_iota(jnp.int32, (tile_height + LANES, reach * tall), 1)
    want = BLOCK_A * (slot % tall) + slot // tall - 1
    want = jnp.where(want < 0, tile_height, jnp.where(want == tile_height, tile_height + 1, want))
    select = (node == want).astype(jnp.float32).astype(jnp.bfloat16)

    def beside(da, db, row):
        return halo_ref[DIRS.index((da, db)), row:row + 1, :]

    for c in range(2):
        own = jnp.transpose(vel_ref[c])
        left = beside(0, -1, 4 * c + 3)[:, :tile_height]
        right = beside(0, 1, 4 * c + 2)[:, :tile_height]
        rest = jnp.zeros((width - tile_width - 2, tile_height), jnp.float32)
        body = jnp.concatenate([own, left, right, rest], axis=0)

        def outer(da, row):
            middle = beside(da, 0, row)[:, :tile_width]
            west = beside(da, -1, row)[:, tile_width - 1:tile_width]
            east = beside(da, 1, row)[:, 0:1]
            return jnp.concatenate(
                [middle, jnp.where(lane == 0, west, jnp.where(lane == 1, east, 0.0))], axis=1)

        ends = jnp.concatenate([outer(-1, 4 * c + 1), outer(1, 4 * c),
                                jnp.zeros((LANES - 2, 2 * LANES), jnp.float32)], axis=0)
        full = jnp.concatenate([body, jnp.transpose(ends)[:width]], axis=1)
        high = rounded(full)
        both = jnp.concatenate([high, full - high], axis=0).astype(jnp.bfloat16)
        spread = jnp.dot(both, select, preferred_element_type=jnp.float32)
        first_half = lax.broadcasted_iota(jnp.int32, (BLOCK_B, LANES), 1) < LANES // 2
        for part in range(2):
            z = spread[part * width:(part + 1) * width]
            plain = [z[:, j * LANES:(j + 1) * LANES] for j in range(reach * tall // LANES)]
            turned = [pltpu.roll(p, LANES // 2, 1) for p in plain]

            def joined(i, rows):
                j, half = i // 2, i % 2
                low, top = (plain[j], turned[j]) if half == 0 else (turned[j], plain[j])
                height = rows[0].stop - rows[0].start
                return jnp.concatenate([jnp.where(first_half[:height], low[rows[2 * k]], top[rows[2 * k + 1]])
                                        for k in range(wide // 2)], axis=1)

            columns = slice(part * tall * wide, (part + 1) * tall * wide)
            for i in range(reach):
                low = (c * reach + i) * BLOCK_B
                table_ref[low:low + BLOCK_B, columns] = joined(
                    i, [slice(BLOCK_B * k, BLOCK_B * (k + 1)) for k in range(wide)]).astype(jnp.bfloat16)
            for e in range(2):
                if e == 0:
                    lines = [tile_width] + [BLOCK_B * k - 1 for k in range(1, wide)]
                else:
                    lines = [BLOCK_B * (k + 1) for k in range(wide - 1)] + [tile_width + 1]
                rows = [joined(i, [slice(r, r + 1) for r in lines]) for i in range(reach)]
                rows.append(jnp.zeros((8 - reach, tall * wide), jnp.float32))
                low = 2 * reach * BLOCK_B + (c * 2 + e) * 8
                table_ref[low:low + 8, columns] = jnp.concatenate(rows, axis=0).astype(jnp.bfloat16)


def gather_nodes(blocks, tile_width, table_ref, nodes_ref):
    cells = jnp.concatenate([b[16 + j:17 + j, :] for b in blocks for j in range(2)], axis=1)
    cell = jnp.maximum(cells, 0.0).astype(jnp.int32)
    row = cell // tile_width
    col = cell - row * tile_width
    index = (col // BLOCK_B) * 64 + row // BLOCK_A
    index = index.astype(jnp.float32).astype(jnp.bfloat16)
    hot = one_hot(narrow_iota((256, index.shape[1]), 0), index)
    nodes_ref[...] = jnp.dot(table_ref[...], jnp.concatenate([hot, hot], axis=0),
                             preferred_element_type=jnp.float32)


def banded(diff, weights):
    return jnp.where(diff == -1, weights[0], jnp.where(diff == 0, weights[1], jnp.where(diff == 1, weights[2], 0.0)))


def weigh(v, cell, tile_width, nodes, weights_ref):
    reach = BLOCK_A + 2
    live = cell >= 0.0
    place = jnp.maximum(cell, 0.0).astype(jnp.int32)
    row = place // tile_width
    col = place - row * tile_width
    row = row % BLOCK_A
    col = col % BLOCK_B
    wa = quad_weights(v[0:1])
    wb = quad_weights(v[1:2])
    aw = banded(lax.broadcasted_iota(jnp.int32, (8, LANES), 0) - 1 - row, wa)
    bw = banded(lax.broadcasted_iota(jnp.int32, (BLOCK_B, LANES), 0) - col, wb)
    left = jnp.where(col == 0, wb[0], 0.0)
    right = jnp.where(col == BLOCK_B - 1, wb[2], 0.0)
    scale = jnp.where(live, step_length, 0.0)
    moved = []
    for c in range(2):
        y = None
        for i in range(reach):
            term = aw[i:i + 1] * nodes(slice((c * reach + i) * BLOCK_B, (c * reach + i + 1) * BLOCK_B))
            y = term if y is None else y + term
        y = y * bw
        low = 2 * reach * BLOCK_B + c * 16
        z = aw * (left * nodes(slice(low, low + 8)) + right * nodes(slice(low + 8, low + 16)))
        for k in range(BLOCK_B // 8):
            z = z + y[8 * k:8 * k + 8]
        moved.append(jnp.sum(z, axis=0, keepdims=True) * scale)
    line = lax.broadcasted_iota(jnp.int32, v.shape, 0)
    return v + jnp.where(line == 2, moved[0], jnp.where(line == 3, moved[1], 0.0))


def advance_block(block, source, at, tile_width, nodes_ref, out_ref, cell_ref):
    for j in range(2):
        lanes = slice(at + j * LANES, at + (j + 1) * LANES)
        v = block[8 * j:8 * j + 8, :]
        cell = block[16 + j:17 + j, :]
        out_ref[:, pl.ds(pl.multiple_of(source * 2 * LANES + j * LANES, LANES), LANES)] = weigh(
            v, cell, tile_width, lambda rows, lanes=lanes: nodes_ref[rows, lanes], None)
    cell_ref[pl.ds(source * 2, 2), :] = block[16:18, :].astype(jnp.int32)


def exchange_kernel(sizes, width, chunk, part_ref, key_ref, a_ref, b_ref, vel_ref, out_ref, cell_ref,
                    hot_ref, base_ref, pick_ref, low_ref, acc_ref, sorted_ref, cells_ref, first_ref, first_smem,
                    outgoing, held, edge_ref, halo_ref, table_ref, nodes_even, nodes_odd,
                    send_sem, recv_sem, halo_send, halo_recv, local_sem):
    nx, ny, nz = sizes
    plane = ny * nz
    n = nx * plane
    tile_height, tile_width = vel_ref.shape[1:]
    gx, gy, gz = lax.axis_index("gx"), lax.axis_index("gy"), lax.axis_index("gz")
    column = gy * nz + gz

    def at(dx, dyz, sign):
        x = lax.rem(gx + sign * dx + nx, nx)
        y = lax.rem(gy + sign * (dyz // nz) + ny, ny)
        z = lax.rem(gz + sign * lax.rem(dyz, nz) + nz, nz)
        return x, y, z

    def linear(place):
        return (place[0] * ny + place[1]) * nz + place[2]

    def halo_copy(k, slot):
        da, db = DIRS[k]
        there = column + db
        return pltpu.make_async_remote_copy(
            src_ref=edge_ref, dst_ref=halo_ref.at[slot], send_sem=halo_send.at[k],
            recv_sem=halo_recv.at[slot], device_id=(gx + da, there // nz, lax.rem(there, nz)),
            device_id_type=pl.DeviceIdType.MESH)

    def exists(k):
        da, db = DIRS[k]
        a, b = gx + da, column + db
        return (a >= 0) & (a < nx) & (b >= 0) & (b < plane)

    def hop(q):
        return lax.rem(q, nx), q // nx

    def block_copy(q):
        there = at(*hop(q), 1)
        return pltpu.make_async_remote_copy(
            src_ref=outgoing.at[q], dst_ref=held.at[q],
            send_sem=send_sem.at[q], recv_sem=recv_sem.at[q], device_id=there,
            device_id_type=pl.DeviceIdType.MESH)

    barrier = pltpu.get_barrier_semaphore()

    def greet(q, carry):
        pl.semaphore_signal(barrier, inc=1, device_id=at(*hop(q), 1), device_id_type=pl.DeviceIdType.MESH)
        return carry

    lax.fori_loop(1, n, greet, 0)
    pack_edges(vel_ref, edge_ref)
    first_ref[...] = jnp.zeros_like(first_ref)
    sort_particles(n, width, chunk, part_ref, key_ref, a_ref, b_ref, hot_ref, base_ref, pick_ref,
                   low_ref, acc_ref, sorted_ref, cells_ref, first_ref)
    to_smem = pltpu.make_async_copy(first_ref, first_smem, local_sem)
    to_smem.start()
    tops = key_ref.shape[1] // width
    tail = tops * width // LANES
    sorted_ref[tail:] = jnp.zeros((3, 8, LANES), jnp.float32)
    cells_ref[tail:] = jnp.zeros((3, 8, LANES), jnp.float32)
    unpack_sorted(tops, width, tile_width, acc_ref, sorted_ref, cells_ref)
    to_smem.wait()
    pl.semaphore_wait(barrier, n - 1)
    for k in range(8):
        @pl.when(exists(k))
        def _(k=k):
            halo_copy(k, 7 - k).start()

        @pl.when(jnp.logical_not(exists(k)))
        def _(k=k):
            halo_ref[k] = jnp.zeros(halo_ref.shape[1:], jnp.float32)

    def cut(q, out):
        owner = linear(at(*hop(q), 1))
        cut_block(first_smem[0, owner], first_smem[1, owner], sorted_ref, cells_ref, out)

    def dispatch(q, carry):
        cut(q, outgoing.at[q])
        block_copy(q).start()
        return carry

    lax.fori_loop(1, n, dispatch, 0)
    cut(0, held.at[0])

    for k in range(8):
        @pl.when(exists(k))
        def _(k=k):
            halo_copy(k, k).wait_recv()

    build_table(vel_ref, halo_ref, table_ref, tile_height, tile_width)

    def gather(t, nodes_ref):
        gather_nodes([held.at[2 * t], held.at[2 * t + 1]], tile_width, table_ref, nodes_ref)

    def weigh_pair(t, nodes_ref):
        for i in range(2):
            source = linear(at(*hop(2 * t + i), -1))
            advance_block(held.at[2 * t + i], source, i * 2 * LANES, tile_width, nodes_ref, out_ref, cell_ref)

    block_copy(1).wait_recv()
    gather(0, nodes_even)

    def both(t, carry):
        block_copy(4 * t + 2).wait_recv()
        block_copy(4 * t + 3).wait_recv()
        gather(2 * t + 1, nodes_odd)
        weigh_pair(2 * t, nodes_even)

        @pl.when(t + 1 < n // 4)
        def _():
            block_copy(4 * t + 4).wait_recv()
            block_copy(4 * t + 5).wait_recv()

        gather(jnp.minimum(2 * t + 2, n // 2 - 1), nodes_even)
        weigh_pair(2 * t + 1, nodes_odd)
        return carry

    lax.fori_loop(0, n // 4, both, 0)

    def sent(q, carry):
        block_copy(q).wait_send()
        return carry

    lax.fori_loop(1, n, sent, 0)
    for k in range(8):
        @pl.when(exists(k))
        def _(k=k):
            halo_copy(k, 7 - k).wait_send()


def shards(particles, dest_key, cell_a, cell_b, velocity):
    owners = lax.axis_size(("gx", "gy", "gz"))
    count = particles.shape[1]
    cap = 4 * count // owners
    tile_height, tile_width = velocity.shape[1:]
    assert owners == LANES and cap == 2 * LANES and (tile_height, tile_width) == (256, 128)
    width, chunk = 256, 1024
    tops = count // width
    sizes = tuple(lax.axis_size(name) for name in ("gx", "gy", "gz"))
    in_vmem = pl.BlockSpec(memory_space=pltpu.VMEM)
    rows = 12 * BLOCK_B + 32
    binned, binned_cell = pl.pallas_call(
        functools.partial(exchange_kernel, sizes, width, chunk),
        out_shape=(jax.ShapeDtypeStruct((8, owners * cap), jnp.float32),
                   jax.ShapeDtypeStruct((owners * 2, LANES), jnp.int32)),
        in_specs=[in_vmem] * 5,
        out_specs=(in_vmem,) * 2,
        scratch_shapes=[
            pltpu.VMEM((owners, count), jnp.bfloat16),
            pltpu.VMEM((tops, owners, LANES), jnp.float32),
            pltpu.VMEM((tops * 18, chunk), jnp.bfloat16),
            pltpu.VMEM((width, chunk), jnp.bfloat16),
            pltpu.VMEM((tops * 18, width), jnp.float32),
            pltpu.VMEM((count // LANES + 3, 8, LANES), jnp.float32),
            pltpu.VMEM((count // LANES + 3, 8, LANES), jnp.float32),
            pltpu.VMEM((8, LANES), jnp.int32),
            pltpu.SMEM((8, LANES), jnp.int32),
            pltpu.VMEM((owners, 18, LANES), jnp.float32),
            pltpu.VMEM((owners, 18, LANES), jnp.float32),
            pltpu.VMEM((8, max(tile_height, tile_width)), jnp.float32),
            pltpu.VMEM((8, 8, max(tile_height, tile_width)), jnp.float32),
            pltpu.VMEM((rows, 2 * 256), jnp.bfloat16),
            pltpu.VMEM((rows, 4 * LANES), jnp.float32),
            pltpu.VMEM((rows, 4 * LANES), jnp.float32),
            pltpu.SemaphoreType.DMA((owners,)),
            pltpu.SemaphoreType.DMA((owners,)),
            pltpu.SemaphoreType.DMA((8,)),
            pltpu.SemaphoreType.DMA((8,)),
            pltpu.SemaphoreType.DMA,
        ],
        compiler_params=pltpu.CompilerParams(collective_id=0, has_side_effects=True),
    )(particles, dest_key.reshape(1, -1), cell_a.reshape(1, -1), cell_b.reshape(1, -1), velocity)
    return (binned, binned_cell.reshape(-1))


def solution(mesh):
    in_specs = (
        P(None, ("gx", "gy", "gz")),
        P(("gx", "gy", "gz")),
        P(("gx", "gy", "gz")),
        P(("gx", "gy", "gz")),
        P(None, "gx", ("gy", "gz")),
    )
    out_specs = (P(None, ("gx", "gy", "gz")), P(("gx", "gy", "gz")))
    return jax.shard_map(shards, mesh=mesh, in_specs=in_specs, out_specs=out_specs, check_vma=False)
```

```python
import functools

import jax
import jax.numpy as jnp
from jax import lax
from jax.experimental import pallas as pl
from jax.experimental.pallas import tpu as pltpu
from jax.sharding import PartitionSpec as P

step_length = 0.5
NT = (((1,), (1,)), ((), ()))
LANES = 128
BLOCK_A, BLOCK_B = 4, 32
DIRS = ((-1, -1), (-1, 0), (-1, 1), (0, -1), (0, 1), (1, -1), (1, 0), (1, 1))


def quad_weights(frac):
    return (0.5 * frac * (frac - 1.0), 1.0 - frac * frac, 0.5 * frac * (frac + 1.0))


def rounded(x):
    return x.astype(jnp.bfloat16).astype(jnp.float32)


def narrow_iota(shape, dim):
    return lax.broadcasted_iota(jnp.int32, shape, dim).astype(jnp.float32).astype(jnp.bfloat16)


def one_hot(row, index):
    one, zero = jnp.ones((), jnp.bfloat16), jnp.zeros((), jnp.bfloat16)
    return jnp.where(row == index, one, zero)


def pack_edges(vel_ref, edge_ref):
    tile_height, tile_width = vel_ref.shape[1:]
    edge_ref[...] = jnp.zeros_like(edge_ref)
    for c in range(2):
        edge_ref[4 * c:4 * c + 1, :tile_width] = vel_ref[c, 0:1, :]
        edge_ref[4 * c + 1:4 * c + 2, :tile_width] = vel_ref[c, tile_height - 1:, :]
        turned = jnp.transpose(vel_ref[c])
        edge_ref[4 * c + 2:4 * c + 3, :tile_height] = turned[0:1]
        edge_ref[4 * c + 3:4 * c + 4, :tile_height] = turned[tile_width - 1:]


def sort_particles(aside, owners, width, chunk, part_ref, key_ref, a_ref, b_ref,
                   hot_ref, base_ref, pick_ref, low_ref, acc_ref, sorted_ref, cells_ref, table_ref):
    count = key_ref.shape[1]
    owner_rows = narrow_iota((owners, width), 0)
    ones = jnp.ones((width, LANES), jnp.bfloat16)
    owner_ids = lax.broadcasted_iota(jnp.int32, (owners, LANES), 0)
    tops = count // width

    def count_chunk(index, carry):
        seen, tally = carry
        aside(index)
        for part in range(chunk // width):
            start = pl.multiple_of(index * chunk + part * width, width)
            keys = key_ref[:, pl.ds(start, width)]
            hot = one_hot(owner_rows, keys.astype(jnp.float32).astype(jnp.bfloat16))
            hot_ref[:, pl.ds(start, width)] = hot
            base_ref[index * (chunk // width) + part] = seen
            seen = seen + jnp.dot(hot, ones, preferred_element_type=jnp.float32)
            for j in range(width // LANES):
                tally = tally + jnp.where(owner_ids == keys[:, j * LANES:(j + 1) * LANES], 1, 0)
        return seen, tally

    total, tally = lax.fori_loop(0, count // chunk, count_chunk, (
        jnp.zeros((owners, LANES), jnp.float32), jnp.zeros((owners, LANES), jnp.int32)))
    tally = jnp.sum(tally, axis=1, keepdims=True)
    below = (lax.broadcasted_iota(jnp.int32, (owners, owners), 1)
             < lax.broadcasted_iota(jnp.int32, (owners, owners), 0)).astype(jnp.float32).astype(jnp.bfloat16)
    first = jnp.dot(below, total.astype(jnp.bfloat16), preferred_element_type=jnp.float32)
    lane_ids = lax.broadcasted_iota(jnp.int32, (owners, LANES), 1)
    table_ref[0:1, :] = jnp.sum(jnp.where(owner_ids < lane_ids, tally, 0), axis=0, keepdims=True)
    table_ref[1:2, :] = jnp.sum(jnp.where(owner_ids == lane_ids, tally, 0), axis=0, keepdims=True)

    upper = (lax.broadcasted_iota(jnp.int32, (width, width), 0)
             < lax.broadcasted_iota(jnp.int32, (width, width), 1)).astype(jnp.float32).astype(jnp.bfloat16)
    low_rows = narrow_iota((width, width), 0)
    top_rows = narrow_iota((tops, width), 0)
    zero = jnp.zeros((), jnp.bfloat16)

    acc_ref[...] = jnp.zeros_like(acc_ref)

    def place_chunk(index, carry):
        for part in range(chunk // width):
            start = pl.multiple_of(index * chunk + part * width, width)
            at = slice(part * width, (part + 1) * width)
            before = jnp.dot(hot_ref[:, pl.ds(start, width)], upper, preferred_element_type=jnp.float32)
            base = base_ref[index * (chunk // width) + part] + first
            keys = key_ref[:, pl.ds(start, width)]
            spots = []
            for j in range(width // LANES):
                cut = slice(j * LANES, (j + 1) * LANES)
                spots.append(jnp.sum(jnp.where(owner_ids == keys[:, cut], before[:, cut] + base, 0.0),
                                     axis=0, keepdims=True))
            spot = jnp.concatenate(spots, axis=1).astype(jnp.int32)
            top_int = spot // width
            top = top_int.astype(jnp.float32).astype(jnp.bfloat16)
            low = (spot - top_int * width).astype(jnp.float32).astype(jnp.bfloat16)
            low_ref[:, at] = one_hot(low_rows, low)
            values = part_ref[:, pl.ds(start, width)]
            high = rounded(values)
            both = jnp.concatenate([high, values - high], axis=0).astype(jnp.bfloat16)
            for i in range(tops):
                pick_ref[i * 16:(i + 1) * 16, at] = jnp.where(top == jnp.full((), i, jnp.bfloat16), both, zero)
            rows = a_ref[:, pl.ds(start, width)].astype(jnp.float32).astype(jnp.bfloat16)
            cols = b_ref[:, pl.ds(start, width)].astype(jnp.float32).astype(jnp.bfloat16)
            mine = top_rows == top
            pick_ref[tops * 16:tops * 17, at] = jnp.where(mine, rows, zero)
            pick_ref[tops * 17:tops * 18, at] = jnp.where(mine, cols, zero)
        acc_ref[...] += lax.dot_general(pick_ref[...], low_ref[...], NT, preferred_element_type=jnp.float32)
        return carry

    lax.fori_loop(0, count // chunk, place_chunk, 0, unroll=2)


def unpack_sorted(tops, width, tile_width, acc_ref, sorted_ref, cells_ref):
    cells = acc_ref[tops * 16:tops * 17, :] * float(tile_width) + acc_ref[tops * 17:tops * 18, :]
    per = width // LANES
    for i in range(tops):
        rows = acc_ref[i * 16:i * 16 + 8, :] + acc_ref[i * 16 + 8:i * 16 + 16, :]
        for j in range(per):
            at = slice(j * LANES, (j + 1) * LANES)
            sorted_ref[i * per + j] = rows[:, at]
            cells_ref[i * per + j, 0:1] = cells[i:i + 1, at]


def cut_block(first, size, sorted_ref, cells_ref, out):
    base = first // LANES
    shift = first - base * LANES
    back = LANES - shift
    lane = lax.broadcasted_iota(jnp.int32, (8, LANES), 1)
    near = lane < back
    turned = [pltpu.roll(sorted_ref[base + j], back, 1) for j in range(3)]
    for j in range(2):
        piece = jnp.where(near, turned[j], turned[j + 1])
        out[8 * j:8 * j + 8, :] = jnp.where(lane + j * LANES < size, piece, 0.0)
    turned = [pltpu.roll(cells_ref[base + j], back, 1) for j in range(3)]
    for j in range(2):
        piece = jnp.where(near, turned[j], turned[j + 1])
        out[16 + j:17 + j, :] = jnp.where(lane + j * LANES < size, piece, -1.0)[0:1]


def build_table(vel_ref, halo_ref, table_ref, tile_height, tile_width):
    width = tile_width + 8
    lane = lax.broadcasted_iota(jnp.int32, (1, LANES), 1)
    tall = tile_height // BLOCK_A
    wide = tile_width // BLOCK_B
    reach = BLOCK_A + 2
    node = lax.broadcasted_iota(jnp.int32, (tile_height + LANES, reach * tall), 0)
    slot = lax.broadcasted_iota(jnp.int32, (tile_height + LANES, reach * tall), 1)
    want = BLOCK_A * (slot % tall) + slot // tall - 1
    want = jnp.where(want < 0, tile_height, jnp.where(want == tile_height, tile_height + 1, want))
    select = (node == want).astype(jnp.float32).astype(jnp.bfloat16)

    def beside(da, db, row):
        return halo_ref[DIRS.index((da, db)), row:row + 1, :]

    for c in range(2):
        own = jnp.transpose(vel_ref[c])
        left = beside(0, -1, 4 * c + 3)[:, :tile_height]
        right = beside(0, 1, 4 * c + 2)[:, :tile_height]
        rest = jnp.zeros((width - tile_width - 2, tile_height), jnp.float32)
        body = jnp.concatenate([own, left, right, rest], axis=0)

        def outer(da, row):
            middle = beside(da, 0, row)[:, :tile_width]
            west = beside(da, -1, row)[:, tile_width - 1:tile_width]
            east = beside(da, 1, row)[:, 0:1]
            return jnp.concatenate(
                [middle, jnp.where(lane == 0, west, jnp.where(lane == 1, east, 0.0))], axis=1)

        ends = jnp.concatenate([outer(-1, 4 * c + 1), outer(1, 4 * c),
                                jnp.zeros((LANES - 2, 2 * LANES), jnp.float32)], axis=0)
        full = jnp.concatenate([body, jnp.transpose(ends)[:width]], axis=1)
        high = rounded(full)
        both = jnp.concatenate([high, full - high], axis=0).astype(jnp.bfloat16)
        spread = jnp.dot(both, select, preferred_element_type=jnp.float32)
        first_half = lax.broadcasted_iota(jnp.int32, (BLOCK_B, LANES), 1) < LANES // 2
        for part in range(2):
            z = spread[part * width:(part + 1) * width]
            plain = [z[:, j * LANES:(j + 1) * LANES] for j in range(reach * tall // LANES)]
            turned = [pltpu.roll(p, LANES // 2, 1) for p in plain]

            def joined(i, rows):
                j, half = i // 2, i % 2
                low, top = (plain[j], turned[j]) if half == 0 else (turned[j], plain[j])
                height = rows[0].stop - rows[0].start
                return jnp.concatenate([jnp.where(first_half[:height], low[rows[2 * k]], top[rows[2 * k + 1]])
                                        for k in range(wide // 2)], axis=1)

            columns = slice(part * tall * wide, (part + 1) * tall * wide)
            for i in range(reach):
                low = (c * reach + i) * BLOCK_B
                table_ref[low:low + BLOCK_B, columns] = joined(
                    i, [slice(BLOCK_B * k, BLOCK_B * (k + 1)) for k in range(wide)]).astype(jnp.bfloat16)
            for e in range(2):
                if e == 0:
                    lines = [tile_width] + [BLOCK_B * k - 1 for k in range(1, wide)]
                else:
                    lines = [BLOCK_B * (k + 1) for k in range(wide - 1)] + [tile_width + 1]
                rows = [joined(i, [slice(r, r + 1) for r in lines]) for i in range(reach)]
                rows.append(jnp.zeros((8 - reach, tall * wide), jnp.float32))
                low = 2 * reach * BLOCK_B + (c * 2 + e) * 8
                table_ref[low:low + 8, columns] = jnp.concatenate(rows, axis=0).astype(jnp.bfloat16)


def gather_nodes(blocks, tile_width, table_ref, nodes_ref):
    cells = jnp.concatenate([b[16 + j:17 + j, :] for b in blocks for j in range(2)], axis=1)
    cell = jnp.maximum(cells, 0.0).astype(jnp.int32)
    row = cell // tile_width
    col = cell - row * tile_width
    index = (col // BLOCK_B) * 64 + row // BLOCK_A
    index = index.astype(jnp.float32).astype(jnp.bfloat16)
    hot = one_hot(narrow_iota((256, index.shape[1]), 0), index)
    nodes_ref[...] = jnp.dot(table_ref[...], jnp.concatenate([hot, hot], axis=0),
                             preferred_element_type=jnp.float32)


def banded(diff, weights):
    return jnp.where(diff == -1, weights[0], jnp.where(diff == 0, weights[1], jnp.where(diff == 1, weights[2], 0.0)))


def weigh(v, cell, tile_width, nodes, weights_ref):
    reach = BLOCK_A + 2
    live = cell >= 0.0
    place = jnp.maximum(cell, 0.0).astype(jnp.int32)
    row = place // tile_width
    col = place - row * tile_width
    row = row % BLOCK_A
    col = col % BLOCK_B
    wa = quad_weights(v[0:1])
    wb = quad_weights(v[1:2])
    aw = banded(lax.broadcasted_iota(jnp.int32, (8, LANES), 0) - 1 - row, wa)
    bw = banded(lax.broadcasted_iota(jnp.int32, (BLOCK_B, LANES), 0) - col, wb)
    left = jnp.where(col == 0, wb[0], 0.0)
    right = jnp.where(col == BLOCK_B - 1, wb[2], 0.0)
    scale = jnp.where(live, step_length, 0.0)
    moved = []
    for c in range(2):
        y = None
        for i in range(reach):
            term = aw[i:i + 1] * nodes(slice((c * reach + i) * BLOCK_B, (c * reach + i + 1) * BLOCK_B))
            y = term if y is None else y + term
        y = y * bw
        low = 2 * reach * BLOCK_B + c * 16
        z = aw * (left * nodes(slice(low, low + 8)) + right * nodes(slice(low + 8, low + 16)))
        for k in range(BLOCK_B // 8):
            z = z + y[8 * k:8 * k + 8]
        moved.append(jnp.sum(z, axis=0, keepdims=True) * scale)
    line = lax.broadcasted_iota(jnp.int32, v.shape, 0)
    return v + jnp.where(line == 2, moved[0], jnp.where(line == 3, moved[1], 0.0))


def advance_block(block, source, at, tile_width, nodes_ref, out_ref, cell_ref):
    for j in range(2):
        lanes = slice(at + j * LANES, at + (j + 1) * LANES)
        v = block[8 * j:8 * j + 8, :]
        cell = block[16 + j:17 + j, :]
        out_ref[:, pl.ds(pl.multiple_of(source * 2 * LANES + j * LANES, LANES), LANES)] = weigh(
            v, cell, tile_width, lambda rows, lanes=lanes: nodes_ref[rows, lanes], None)
    cell_ref[pl.ds(source * 2, 2), :] = block[16:18, :].astype(jnp.int32)


def exchange_kernel(sizes, width, chunk, part_ref, key_ref, a_ref, b_ref, vel_ref, out_ref, cell_ref,
                    hot_ref, base_ref, pick_ref, low_ref, acc_ref, sorted_ref, cells_ref, first_ref, first_smem,
                    outgoing, held, edge_ref, halo_ref, table_ref, nodes_even, nodes_odd,
                    send_sem, recv_sem, halo_send, halo_recv, local_sem):
    nx, ny, nz = sizes
    plane = ny * nz
    n = nx * plane
    tile_height, tile_width = vel_ref.shape[1:]
    gx, gy, gz = lax.axis_index("gx"), lax.axis_index("gy"), lax.axis_index("gz")
    column = gy * nz + gz

    def at(dx, dyz, sign):
        x = lax.rem(gx + sign * dx + nx, nx)
        y = lax.rem(gy + sign * (dyz // nz) + ny, ny)
        z = lax.rem(gz + sign * lax.rem(dyz, nz) + nz, nz)
        return x, y, z

    def linear(place):
        return (place[0] * ny + place[1]) * nz + place[2]

    def halo_copy(k, slot):
        da, db = DIRS[k]
        there = column + db
        return pltpu.make_async_remote_copy(
            src_ref=edge_ref, dst_ref=halo_ref.at[slot], send_sem=halo_send.at[k],
            recv_sem=halo_recv.at[slot], device_id=(gx + da, there // nz, lax.rem(there, nz)),
            device_id_type=pl.DeviceIdType.MESH)

    def exists(k):
        da, db = DIRS[k]
        a, b = gx + da, column + db
        return (a >= 0) & (a < nx) & (b >= 0) & (b < plane)

    def hop(q):
        core, r = lax.rem(q, nz), q // nz
        z = lax.rem(r, nx)
        x = lax.rem(r + r // nx, 4)
        y = lax.rem(r + r // (4 * nx), ny // 4)
        return z, (y * 4 + x) * nz + core

    def block_copy(q):
        there = at(*hop(q), 1)
        return pltpu.make_async_remote_copy(
            src_ref=outgoing.at[q], dst_ref=held.at[q],
            send_sem=send_sem.at[q], recv_sem=recv_sem.at[q], device_id=there,
            device_id_type=pl.DeviceIdType.MESH)

    barrier = pltpu.get_barrier_semaphore()

    def greet(q, carry):
        pl.semaphore_signal(barrier, inc=1, device_id=at(*hop(q), 1), device_id_type=pl.DeviceIdType.MESH)
        return carry

    share = (n - 1) // 8
    lax.fori_loop(8 * share + 1, n, greet, 0)

    def greet_some(index):
        for i in range(share):
            greet(index * share + i + 1, 0)

    pack_edges(vel_ref, edge_ref)
    first_ref[...] = jnp.zeros_like(first_ref)
    sort_particles(greet_some, n, width, chunk, part_ref, key_ref, a_ref, b_ref, hot_ref, base_ref, pick_ref,
                   low_ref, acc_ref, sorted_ref, cells_ref, first_ref)
    to_smem = pltpu.make_async_copy(first_ref, first_smem, local_sem)
    to_smem.start()
    tops = key_ref.shape[1] // width
    tail = tops * width // LANES
    sorted_ref[tail:] = jnp.zeros((3, 8, LANES), jnp.float32)
    cells_ref[tail:] = jnp.zeros((3, 8, LANES), jnp.float32)
    unpack_sorted(tops, width, tile_width, acc_ref, sorted_ref, cells_ref)
    to_smem.wait()
    pl.semaphore_wait(barrier, n - 1)
    for k in range(8):
        @pl.when(exists(k))
        def _(k=k):
            halo_copy(k, 7 - k).start()

        @pl.when(jnp.logical_not(exists(k)))
        def _(k=k):
            halo_ref[k] = jnp.zeros(halo_ref.shape[1:], jnp.float32)

    def dispatch(p, carry):
        for i in range(8):
            q = p * 8 + i
            owner = linear(at(*hop(q), 1))
            cut_block(first_smem[0, owner], first_smem[1, owner], sorted_ref, cells_ref, outgoing.at[q])

        @pl.when(p > 0)
        def _():
            block_copy(p * 8).start()

        for i in range(1, 8):
            block_copy(p * 8 + i).start()
        return carry

    lax.fori_loop(0, n // 8, dispatch, 0)
    held[0] = outgoing[0]

    for k in range(8):
        @pl.when(exists(k))
        def _(k=k):
            halo_copy(k, k).wait_recv()

    build_table(vel_ref, halo_ref, table_ref, tile_height, tile_width)

    def gather(t, nodes_ref):
        gather_nodes([held.at[2 * t], held.at[2 * t + 1]], tile_width, table_ref, nodes_ref)

    def weigh_pair(t, nodes_ref):
        for i in range(2):
            source = linear(at(*hop(2 * t + i), -1))
            advance_block(held.at[2 * t + i], source, i * 2 * LANES, tile_width, nodes_ref, out_ref, cell_ref)

    group = 16
    block_copy(1).wait_recv()
    gather(0, nodes_even)

    def arrive(q, carry):
        block_copy(q).wait_recv()
        return carry

    def one_group(p, carry):
        lax.fori_loop(p * group + 2, jnp.minimum((p + 1) * group + 2, n), arrive, 0)
        first = p * (group // 2)

        for t in range(group // 4):
            gather(first + 2 * t + 1, nodes_odd)
            weigh_pair(first + 2 * t, nodes_even)
            gather(jnp.minimum(first + 2 * t + 2, n // 2 - 1), nodes_even)
            weigh_pair(first + 2 * t + 1, nodes_odd)
        return carry

    lax.fori_loop(0, n // group, one_group, 0)

    def sent(q, carry):
        block_copy(q).wait_send()
        return carry

    lax.fori_loop(1, n, sent, 0)
    for k in range(8):
        @pl.when(exists(k))
        def _(k=k):
            halo_copy(k, 7 - k).wait_send()


def shards(particles, dest_key, cell_a, cell_b, velocity):
    owners = lax.axis_size(("gx", "gy", "gz"))
    count = particles.shape[1]
    cap = 4 * count // owners
    tile_height, tile_width = velocity.shape[1:]
    assert owners == LANES and cap == 2 * LANES and (tile_height, tile_width) == (256, 128)
    width, chunk = 256, 1024
    tops = count // width
    sizes = tuple(lax.axis_size(name) for name in ("gx", "gy", "gz"))
    in_vmem = pl.BlockSpec(memory_space=pltpu.VMEM)
    rows = 12 * BLOCK_B + 32
    binned, binned_cell = pl.pallas_call(
        functools.partial(exchange_kernel, sizes, width, chunk),
        out_shape=(jax.ShapeDtypeStruct((8, owners * cap), jnp.float32),
                   jax.ShapeDtypeStruct((owners * 2, LANES), jnp.int32)),
        in_specs=[in_vmem] * 5,
        out_specs=(in_vmem,) * 2,
        scratch_shapes=[
            pltpu.VMEM((owners, count), jnp.bfloat16),
            pltpu.VMEM((tops, owners, LANES), jnp.float32),
            pltpu.VMEM((tops * 18, chunk), jnp.bfloat16),
            pltpu.VMEM((width, chunk), jnp.bfloat16),
            pltpu.VMEM((tops * 18, width), jnp.float32),
            pltpu.VMEM((count // LANES + 3, 8, LANES), jnp.float32),
            pltpu.VMEM((count // LANES + 3, 8, LANES), jnp.float32),
            pltpu.VMEM((8, LANES), jnp.int32),
            pltpu.SMEM((8, LANES), jnp.int32),
            pltpu.VMEM((owners, 18, LANES), jnp.float32),
            pltpu.VMEM((owners, 18, LANES), jnp.float32),
            pltpu.VMEM((8, max(tile_height, tile_width)), jnp.float32),
            pltpu.VMEM((8, 8, max(tile_height, tile_width)), jnp.float32),
            pltpu.VMEM((rows, 2 * 256), jnp.bfloat16),
            pltpu.VMEM((rows, 4 * LANES), jnp.float32),
            pltpu.VMEM((rows, 4 * LANES), jnp.float32),
            pltpu.SemaphoreType.DMA((owners,)),
            pltpu.SemaphoreType.DMA((owners,)),
            pltpu.SemaphoreType.DMA((8,)),
            pltpu.SemaphoreType.DMA((8,)),
            pltpu.SemaphoreType.DMA,
        ],
        compiler_params=pltpu.CompilerParams(collective_id=0, has_side_effects=True),
    )(particles, dest_key.reshape(1, -1), cell_a.reshape(1, -1), cell_b.reshape(1, -1), velocity)
    return (binned, binned_cell.reshape(-1))


def solution(mesh):
    in_specs = (
        P(None, ("gx", "gy", "gz")),
        P(("gx", "gy", "gz")),
        P(("gx", "gy", "gz")),
        P(("gx", "gy", "gz")),
        P(None, "gx", ("gy", "gz")),
    )
    out_specs = (P(None, ("gx", "gy", "gz")), P(("gx", "gy", "gz")))
    return jax.shard_map(shards, mesh=mesh, in_specs=in_specs, out_specs=out_specs, check_vma=False)
```

```python
import functools

import jax
import jax.numpy as jnp
from jax import lax
from jax.experimental import pallas as pl
from jax.experimental.pallas import tpu as pltpu
from jax.sharding import PartitionSpec as P

step_length = 0.5
NT = (((1,), (1,)), ((), ()))
LANES = 128
BLOCK_A, BLOCK_B = 4, 32
DIRS = ((-1, -1), (-1, 0), (-1, 1), (0, -1), (0, 1), (1, -1), (1, 0), (1, 1))


def quad_weights(frac):
    return (0.5 * frac * (frac - 1.0), 1.0 - frac * frac, 0.5 * frac * (frac + 1.0))


def rounded(x):
    return x.astype(jnp.bfloat16).astype(jnp.float32)


def narrow_iota(shape, dim):
    return lax.broadcasted_iota(jnp.int32, shape, dim).astype(jnp.float32).astype(jnp.bfloat16)


def one_hot(row, index):
    one, zero = jnp.ones((), jnp.bfloat16), jnp.zeros((), jnp.bfloat16)
    return jnp.where(row == index, one, zero)


def pack_edges(vel_ref, edge_ref):
    tile_height, tile_width = vel_ref.shape[1:]
    edge_ref[...] = jnp.zeros_like(edge_ref)
    for c in range(2):
        edge_ref[4 * c:4 * c + 1, :tile_width] = vel_ref[c, 0:1, :]
        edge_ref[4 * c + 1:4 * c + 2, :tile_width] = vel_ref[c, tile_height - 1:, :]
        turned = jnp.transpose(vel_ref[c])
        edge_ref[4 * c + 2:4 * c + 3, :tile_height] = turned[0:1]
        edge_ref[4 * c + 3:4 * c + 4, :tile_height] = turned[tile_width - 1:]


def sort_particles(aside, owners, width, chunk, part_ref, key_ref, a_ref, b_ref,
                   hot_ref, base_ref, pick_ref, low_ref, acc_ref, sorted_ref, cells_ref, table_ref):
    count = key_ref.shape[1]
    owner_rows = narrow_iota((owners, width), 0)
    ones = jnp.ones((width, LANES), jnp.bfloat16)
    owner_ids = lax.broadcasted_iota(jnp.int32, (owners, LANES), 0)
    tops = count // width

    def count_chunk(index, carry):
        seen, tally = carry
        for part in range(chunk // width):
            start = pl.multiple_of(index * chunk + part * width, width)
            keys = key_ref[:, pl.ds(start, width)]
            hot = one_hot(owner_rows, keys.astype(jnp.float32).astype(jnp.bfloat16))
            hot_ref[:, pl.ds(start, width)] = hot
            base_ref[index * (chunk // width) + part] = seen
            seen = seen + jnp.dot(hot, ones, preferred_element_type=jnp.float32)
            for j in range(width // LANES):
                tally = tally + jnp.where(owner_ids == keys[:, j * LANES:(j + 1) * LANES], 1, 0)
        return seen, tally

    total, tally = lax.fori_loop(0, count // chunk, count_chunk, (
        jnp.zeros((owners, LANES), jnp.float32), jnp.zeros((owners, LANES), jnp.int32)))
    tally = jnp.sum(tally, axis=1, keepdims=True)
    below = (lax.broadcasted_iota(jnp.int32, (owners, owners), 1)
             < lax.broadcasted_iota(jnp.int32, (owners, owners), 0)).astype(jnp.float32).astype(jnp.bfloat16)
    first = jnp.dot(below, total.astype(jnp.bfloat16), preferred_element_type=jnp.float32)
    lane_ids = lax.broadcasted_iota(jnp.int32, (owners, LANES), 1)
    table_ref[0:1, :] = jnp.sum(jnp.where(owner_ids < lane_ids, tally, 0), axis=0, keepdims=True)
    table_ref[1:2, :] = jnp.sum(jnp.where(owner_ids == lane_ids, tally, 0), axis=0, keepdims=True)

    upper = (lax.broadcasted_iota(jnp.int32, (width, width), 0)
             < lax.broadcasted_iota(jnp.int32, (width, width), 1)).astype(jnp.float32).astype(jnp.bfloat16)
    low_rows = narrow_iota((width, width), 0)
    top_rows = narrow_iota((tops, width), 0)
    zero = jnp.zeros((), jnp.bfloat16)

    acc_ref[...] = jnp.zeros_like(acc_ref)

    def place_chunk(index, carry):
        for part in range(chunk // width):
            start = pl.multiple_of(index * chunk + part * width, width)
            at = slice(part * width, (part + 1) * width)
            before = jnp.dot(hot_ref[:, pl.ds(start, width)], upper, preferred_element_type=jnp.float32)
            base = base_ref[index * (chunk // width) + part] + first
            keys = key_ref[:, pl.ds(start, width)]
            spots = []
            for j in range(width // LANES):
                cut = slice(j * LANES, (j + 1) * LANES)
                spots.append(jnp.sum(jnp.where(owner_ids == keys[:, cut], before[:, cut] + base, 0.0),
                                     axis=0, keepdims=True))
            spot = jnp.concatenate(spots, axis=1).astype(jnp.int32)
            top_int = spot // width
            top = top_int.astype(jnp.float32).astype(jnp.bfloat16)
            low = (spot - top_int * width).astype(jnp.float32).astype(jnp.bfloat16)
            low_ref[:, at] = one_hot(low_rows, low)
            values = part_ref[:, pl.ds(start, width)]
            high = rounded(values)
            both = jnp.concatenate([high, values - high], axis=0).astype(jnp.bfloat16)
            for i in range(tops):
                pick_ref[i * 16:(i + 1) * 16, at] = jnp.where(top == jnp.full((), i, jnp.bfloat16), both, zero)
            rows = a_ref[:, pl.ds(start, width)].astype(jnp.float32).astype(jnp.bfloat16)
            cols = b_ref[:, pl.ds(start, width)].astype(jnp.float32).astype(jnp.bfloat16)
            mine = top_rows == top
            pick_ref[tops * 16:tops * 17, at] = jnp.where(mine, rows, zero)
            pick_ref[tops * 17:tops * 18, at] = jnp.where(mine, cols, zero)
        acc_ref[...] += lax.dot_general(pick_ref[...], low_ref[...], NT, preferred_element_type=jnp.float32)
        return carry

    half = count // chunk // 2
    lax.fori_loop(0, half, place_chunk, 0, unroll=2)
    aside()
    lax.fori_loop(half, 2 * half, place_chunk, 0, unroll=2)


def unpack_sorted(tops, width, tile_width, acc_ref, sorted_ref, cells_ref):
    cells = acc_ref[tops * 16:tops * 17, :] * float(tile_width) + acc_ref[tops * 17:tops * 18, :]
    per = width // LANES
    for i in range(tops):
        rows = acc_ref[i * 16:i * 16 + 8, :] + acc_ref[i * 16 + 8:i * 16 + 16, :]
        for j in range(per):
            at = slice(j * LANES, (j + 1) * LANES)
            sorted_ref[i * per + j] = rows[:, at]
            cells_ref[i * per + j, 0:1] = cells[i:i + 1, at]


def cut_block(first, size, sorted_ref, cells_ref, out):
    base = first // LANES
    shift = first - base * LANES
    back = LANES - shift
    lane = lax.broadcasted_iota(jnp.int32, (8, LANES), 1)
    near = lane < back
    turned = [pltpu.roll(sorted_ref[base + j], back, 1) for j in range(3)]
    for j in range(2):
        piece = jnp.where(near, turned[j], turned[j + 1])
        out[8 * j:8 * j + 8, :] = jnp.where(lane + j * LANES < size, piece, 0.0)
    turned = [pltpu.roll(cells_ref[base + j], back, 1) for j in range(3)]
    for j in range(2):
        piece = jnp.where(near, turned[j], turned[j + 1])
        out[16 + j:17 + j, :] = jnp.where(lane + j * LANES < size, piece, -1.0)[0:1]


def build_table(vel_ref, halo_ref, table_ref, tile_height, tile_width):
    width = tile_width + 8
    lane = lax.broadcasted_iota(jnp.int32, (1, LANES), 1)
    tall = tile_height // BLOCK_A
    wide = tile_width // BLOCK_B
    reach = BLOCK_A + 2
    node = lax.broadcasted_iota(jnp.int32, (tile_height + LANES, reach * tall), 0)
    slot = lax.broadcasted_iota(jnp.int32, (tile_height + LANES, reach * tall), 1)
    want = BLOCK_A * (slot % tall) + slot // tall - 1
    want = jnp.where(want < 0, tile_height, jnp.where(want == tile_height, tile_height + 1, want))
    select = (node == want).astype(jnp.float32).astype(jnp.bfloat16)

    def beside(da, db, row):
        return halo_ref[DIRS.index((da, db)), row:row + 1, :]

    for c in range(2):
        own = jnp.transpose(vel_ref[c])
        left = beside(0, -1, 4 * c + 3)[:, :tile_height]
        right = beside(0, 1, 4 * c + 2)[:, :tile_height]
        rest = jnp.zeros((width - tile_width - 2, tile_height), jnp.float32)
        body = jnp.concatenate([own, left, right, rest], axis=0)

        def outer(da, row):
            middle = beside(da, 0, row)[:, :tile_width]
            west = beside(da, -1, row)[:, tile_width - 1:tile_width]
            east = beside(da, 1, row)[:, 0:1]
            return jnp.concatenate(
                [middle, jnp.where(lane == 0, west, jnp.where(lane == 1, east, 0.0))], axis=1)

        ends = jnp.concatenate([outer(-1, 4 * c + 1), outer(1, 4 * c),
                                jnp.zeros((LANES - 2, 2 * LANES), jnp.float32)], axis=0)
        full = jnp.concatenate([body, jnp.transpose(ends)[:width]], axis=1)
        high = rounded(full)
        both = jnp.concatenate([high, full - high], axis=0).astype(jnp.bfloat16)
        spread = jnp.dot(both, select, preferred_element_type=jnp.float32)
        first_half = lax.broadcasted_iota(jnp.int32, (BLOCK_B, LANES), 1) < LANES // 2
        for part in range(2):
            z = spread[part * width:(part + 1) * width]
            plain = [z[:, j * LANES:(j + 1) * LANES] for j in range(reach * tall // LANES)]
            turned = [pltpu.roll(p, LANES // 2, 1) for p in plain]

            def joined(i, rows):
                j, half = i // 2, i % 2
                low, top = (plain[j], turned[j]) if half == 0 else (turned[j], plain[j])
                height = rows[0].stop - rows[0].start
                return jnp.concatenate([jnp.where(first_half[:height], low[rows[2 * k]], top[rows[2 * k + 1]])
                                        for k in range(wide // 2)], axis=1)

            columns = slice(part * tall * wide, (part + 1) * tall * wide)
            for i in range(reach):
                low = (c * reach + i) * BLOCK_B
                table_ref[low:low + BLOCK_B, columns] = joined(
                    i, [slice(BLOCK_B * k, BLOCK_B * (k + 1)) for k in range(wide)]).astype(jnp.bfloat16)
            for e in range(2):
                if e == 0:
                    lines = [tile_width] + [BLOCK_B * k - 1 for k in range(1, wide)]
                else:
                    lines = [BLOCK_B * (k + 1) for k in range(wide - 1)] + [tile_width + 1]
                rows = [joined(i, [slice(r, r + 1) for r in lines]) for i in range(reach)]
                rows.append(jnp.zeros((8 - reach, tall * wide), jnp.float32))
                low = 2 * reach * BLOCK_B + (c * 2 + e) * 8
                table_ref[low:low + 8, columns] = jnp.concatenate(rows, axis=0).astype(jnp.bfloat16)


def gather_nodes(blocks, tile_width, table_ref, nodes_ref):
    cells = jnp.concatenate([b[16 + j:17 + j, :] for b in blocks for j in range(2)], axis=1)
    cell = jnp.maximum(cells, 0.0).astype(jnp.int32)
    row = cell // tile_width
    col = cell - row * tile_width
    index = (col // BLOCK_B) * 64 + row // BLOCK_A
    index = index.astype(jnp.float32).astype(jnp.bfloat16)
    hot = one_hot(narrow_iota((256, index.shape[1]), 0), index)
    nodes_ref[...] = jnp.dot(table_ref[...], jnp.concatenate([hot, hot], axis=0),
                             preferred_element_type=jnp.float32)


def banded(diff, weights):
    return jnp.where(diff == -1, weights[0], jnp.where(diff == 0, weights[1], jnp.where(diff == 1, weights[2], 0.0)))


def weigh(v, cell, tile_width, nodes, weights_ref):
    reach = BLOCK_A + 2
    live = cell >= 0.0
    place = jnp.maximum(cell, 0.0).astype(jnp.int32)
    row = place // tile_width
    col = place - row * tile_width
    row = row % BLOCK_A
    col = col % BLOCK_B
    wa = quad_weights(v[0:1])
    wb = quad_weights(v[1:2])
    aw = banded(lax.broadcasted_iota(jnp.int32, (8, LANES), 0) - 1 - row, wa)
    bw = banded(lax.broadcasted_iota(jnp.int32, (BLOCK_B, LANES), 0) - col, wb)
    left = jnp.where(col == 0, wb[0], 0.0)
    right = jnp.where(col == BLOCK_B - 1, wb[2], 0.0)
    scale = jnp.where(live, step_length, 0.0)
    moved = []
    for c in range(2):
        y = None
        for i in range(reach):
            term = aw[i:i + 1] * nodes(slice((c * reach + i) * BLOCK_B, (c * reach + i + 1) * BLOCK_B))
            y = term if y is None else y + term
        y = y * bw
        low = 2 * reach * BLOCK_B + c * 16
        z = aw * (left * nodes(slice(low, low + 8)) + right * nodes(slice(low + 8, low + 16)))
        for k in range(BLOCK_B // 8):
            z = z + y[8 * k:8 * k + 8]
        moved.append(jnp.sum(z, axis=0, keepdims=True) * scale)
    line = lax.broadcasted_iota(jnp.int32, v.shape, 0)
    return v + jnp.where(line == 2, moved[0], jnp.where(line == 3, moved[1], 0.0))


def advance_block(block, source, at, tile_width, nodes_ref, out_ref, cell_ref):
    for j in range(2):
        lanes = slice(at + j * LANES, at + (j + 1) * LANES)
        v = block[8 * j:8 * j + 8, :]
        cell = block[16 + j:17 + j, :]
        out_ref[:, pl.ds(pl.multiple_of(source * 2 * LANES + j * LANES, LANES), LANES)] = weigh(
            v, cell, tile_width, lambda rows, lanes=lanes: nodes_ref[rows, lanes], None)
    cell_ref[pl.ds(source * 2, 2), :] = block[16:18, :].astype(jnp.int32)


def exchange_kernel(sizes, width, chunk, part_ref, key_ref, a_ref, b_ref, vel_ref, out_ref, cell_ref,
                    hot_ref, base_ref, pick_ref, low_ref, acc_ref, sorted_ref, cells_ref, first_ref, first_smem,
                    outgoing, held, edge_ref, halo_ref, table_ref, nodes_even, nodes_odd,
                    send_sem, recv_sem, halo_send, halo_recv, local_sem, row_sem):
    nx, ny, nz = sizes
    plane = ny * nz
    n = nx * plane
    group = 16
    tile_height, tile_width = vel_ref.shape[1:]
    gx, gy, gz = lax.axis_index("gx"), lax.axis_index("gy"), lax.axis_index("gz")
    column = gy * nz + gz

    assert (nx, ny, nz) == (4, 16, 2)

    def at(dx, dyz, sign):
        x = (gx + sign * dx) & (nx - 1)
        y = (gy + sign * (dyz >> 1)) & (ny - 1)
        z = gz ^ (dyz & 1)
        return x, y, z

    def linear(place):
        return (place[0] * ny + place[1]) * nz + place[2]

    def halo_copy(k, slot):
        da, db = DIRS[k]
        there = column + db
        return pltpu.make_async_remote_copy(
            src_ref=edge_ref, dst_ref=halo_ref.at[slot], send_sem=halo_send.at[k],
            recv_sem=halo_recv.at[slot], device_id=(gx + da, there // nz, lax.rem(there, nz)),
            device_id_type=pl.DeviceIdType.MESH)

    def exists(k):
        da, db = DIRS[k]
        a, b = gx + da, column + db
        return (a >= 0) & (a < nx) & (b >= 0) & (b < plane)

    def hop(q):
        core, r = q & 1, q >> 1
        z = r & 3
        x = (r + (r >> 2)) & 3
        y = (r + (r >> 4)) & 3
        return z, (y * 4 + x) * nz + core

    def block_copy(q):
        return pltpu.make_async_remote_copy(
            src_ref=outgoing.at[q], dst_ref=held.at[q],
            send_sem=send_sem, recv_sem=recv_sem.at[(q + group - 2) >> 4], device_id=at(*hop(q), 1),
            device_id_type=pl.DeviceIdType.MESH)

    def arrived(first, size, p):
        some = pl.ds(first, size)
        return pltpu.make_async_remote_copy(
            src_ref=outgoing.at[some], dst_ref=held.at[some], send_sem=send_sem, recv_sem=recv_sem.at[p],
            device_id=at(*hop(1), 1), device_id_type=pl.DeviceIdType.MESH)

    barrier = pltpu.get_barrier_semaphore()

    def row_peer(i):
        return (gx + (i >> 1)) & (nx - 1), gy, gz ^ (i & 1)

    def greet(i, carry):
        pl.semaphore_signal(barrier, inc=1, device_id=(gx, (gy + i) & (ny - 1), gz),
                            device_id_type=pl.DeviceIdType.MESH)
        return carry

    lax.fori_loop(1, ny, greet, 0)
    for i in range(1, nx * nz):
        pl.semaphore_signal(barrier, inc=1, device_id=row_peer(i), device_id_type=pl.DeviceIdType.MESH)

    def pass_on():
        pl.semaphore_wait(barrier, ny - 1 + nx * nz - 1)
        for i in range(1, nx * nz):
            pl.semaphore_signal(row_sem, inc=1, device_id=row_peer(i), device_id_type=pl.DeviceIdType.MESH)

    pack_edges(vel_ref, edge_ref)
    first_ref[...] = jnp.zeros_like(first_ref)
    sort_particles(pass_on, n, width, chunk, part_ref, key_ref, a_ref, b_ref, hot_ref, base_ref, pick_ref,
                   low_ref, acc_ref, sorted_ref, cells_ref, first_ref)
    to_smem = pltpu.make_async_copy(first_ref, first_smem, local_sem)
    to_smem.start()
    tops = key_ref.shape[1] // width
    tail = tops * width // LANES
    sorted_ref[tail:] = jnp.zeros((3, 8, LANES), jnp.float32)
    cells_ref[tail:] = jnp.zeros((3, 8, LANES), jnp.float32)
    unpack_sorted(tops, width, tile_width, acc_ref, sorted_ref, cells_ref)
    to_smem.wait()
    pl.semaphore_wait(row_sem, nx * nz - 1)
    for k in range(8):
        @pl.when(exists(k))
        def _(k=k):
            halo_copy(k, 7 - k).start()

        @pl.when(jnp.logical_not(exists(k)))
        def _(k=k):
            halo_ref[k] = jnp.zeros(halo_ref.shape[1:], jnp.float32)

    def dispatch(p, carry):
        for i in range(8):
            q = p * 8 + i
            owner = linear(at(*hop(q), 1))
            cut_block(first_smem[0, owner], first_smem[1, owner], sorted_ref, cells_ref, outgoing.at[q])

        @pl.when(p > 0)
        def _():
            block_copy(p * 8).start()

        for i in range(1, 8):
            block_copy(p * 8 + i).start()
        return carry

    lax.fori_loop(0, n // 8, dispatch, 0)
    held[0] = outgoing[0]

    for k in range(8):
        @pl.when(exists(k))
        def _(k=k):
            halo_copy(k, k).wait_recv()

    build_table(vel_ref, halo_ref, table_ref, tile_height, tile_width)

    def gather(t, nodes_ref):
        gather_nodes([held.at[2 * t], held.at[2 * t + 1]], tile_width, table_ref, nodes_ref)

    def weigh_pair(t, nodes_ref):
        for i in range(2):
            source = linear(at(*hop(2 * t + i), -1))
            advance_block(held.at[2 * t + i], source, i * 2 * LANES, tile_width, nodes_ref, out_ref, cell_ref)

    arrived(1, 1, 0).wait_recv()
    gather(0, nodes_even)

    def one_group(p, carry):
        @pl.when(p < n // group - 1)
        def _():
            arrived(p * group + 2, group, p + 1).wait_recv()

        @pl.when(p == n // group - 1)
        def _():
            arrived(n - group + 2, group - 2, n // group).wait_recv()

        first = p * (group // 2)

        for t in range(group // 4):
            gather(first + 2 * t + 1, nodes_odd)
            weigh_pair(first + 2 * t, nodes_even)
            gather(jnp.minimum(first + 2 * t + 2, n // 2 - 1), nodes_even)
            weigh_pair(first + 2 * t + 1, nodes_odd)
        return carry

    lax.fori_loop(0, n // group, one_group, 0)

    arrived(1, n - 1, 0).wait_send()
    for k in range(8):
        @pl.when(exists(k))
        def _(k=k):
            halo_copy(k, 7 - k).wait_send()


def shards(particles, dest_key, cell_a, cell_b, velocity):
    owners = lax.axis_size(("gx", "gy", "gz"))
    count = particles.shape[1]
    cap = 4 * count // owners
    tile_height, tile_width = velocity.shape[1:]
    assert owners == LANES and cap == 2 * LANES and (tile_height, tile_width) == (256, 128)
    width, chunk = 256, 1024
    tops = count // width
    sizes = tuple(lax.axis_size(name) for name in ("gx", "gy", "gz"))
    in_vmem = pl.BlockSpec(memory_space=pltpu.VMEM)
    rows = 12 * BLOCK_B + 32
    binned, binned_cell = pl.pallas_call(
        functools.partial(exchange_kernel, sizes, width, chunk),
        out_shape=(jax.ShapeDtypeStruct((8, owners * cap), jnp.float32),
                   jax.ShapeDtypeStruct((owners * 2, LANES), jnp.int32)),
        in_specs=[in_vmem] * 5,
        out_specs=(in_vmem,) * 2,
        scratch_shapes=[
            pltpu.VMEM((owners, count), jnp.bfloat16),
            pltpu.VMEM((tops, owners, LANES), jnp.float32),
            pltpu.VMEM((tops * 18, chunk), jnp.bfloat16),
            pltpu.VMEM((width, chunk), jnp.bfloat16),
            pltpu.VMEM((tops * 18, width), jnp.float32),
            pltpu.VMEM((count // LANES + 3, 8, LANES), jnp.float32),
            pltpu.VMEM((count // LANES + 3, 8, LANES), jnp.float32),
            pltpu.VMEM((8, LANES), jnp.int32),
            pltpu.SMEM((8, LANES), jnp.int32),
            pltpu.VMEM((owners, 18, LANES), jnp.float32),
            pltpu.VMEM((owners, 18, LANES), jnp.float32),
            pltpu.VMEM((8, max(tile_height, tile_width)), jnp.float32),
            pltpu.VMEM((8, 8, max(tile_height, tile_width)), jnp.float32),
            pltpu.VMEM((rows, 2 * 256), jnp.bfloat16),
            pltpu.VMEM((rows, 4 * LANES), jnp.float32),
            pltpu.VMEM((rows, 4 * LANES), jnp.float32),
            pltpu.SemaphoreType.DMA,
            pltpu.SemaphoreType.DMA((owners // 16 + 1,)),
            pltpu.SemaphoreType.DMA((8,)),
            pltpu.SemaphoreType.DMA((8,)),
            pltpu.SemaphoreType.DMA,
            pltpu.SemaphoreType.REGULAR,
        ],
        compiler_params=pltpu.CompilerParams(collective_id=0, has_side_effects=True),
    )(particles, dest_key.reshape(1, -1), cell_a.reshape(1, -1), cell_b.reshape(1, -1), velocity)
    return (binned, binned_cell.reshape(-1))


def solution(mesh):
    in_specs = (
        P(None, ("gx", "gy", "gz")),
        P(("gx", "gy", "gz")),
        P(("gx", "gy", "gz")),
        P(("gx", "gy", "gz")),
        P(None, "gx", ("gy", "gz")),
    )
    out_specs = (P(None, ("gx", "gy", "gz")), P(("gx", "gy", "gz")))
    return jax.shard_map(shards, mesh=mesh, in_specs=in_specs, out_specs=out_specs, check_vma=False)
```

```python
import functools

import jax
import jax.numpy as jnp
from jax import lax
from jax.experimental import pallas as pl
from jax.experimental.pallas import tpu as pltpu
from jax.sharding import PartitionSpec as P

step_length = 0.5
NT = (((1,), (1,)), ((), ()))
LANES = 128
NARROW = jnp.float8_e4m3fn
TERMS, TOP = 3, 256.0
BLOCK_A, BLOCK_B = 4, 32
DIRS = ((-1, -1), (-1, 0), (-1, 1), (0, -1), (0, 1), (1, -1), (1, 0), (1, 1))


def quad_weights(frac):
    return (0.5 * frac * (frac - 1.0), 1.0 - frac * frac, 0.5 * frac * (frac + 1.0))


def rounded(x):
    return x.astype(jnp.bfloat16).astype(jnp.float32)


def narrow_iota(shape, dim):
    return lax.broadcasted_iota(jnp.int32, shape, dim).astype(jnp.float32).astype(jnp.bfloat16)


def one_hot(row, index):
    one, zero = jnp.ones((), jnp.bfloat16), jnp.zeros((), jnp.bfloat16)
    return jnp.where(row == index, one, zero)


def pack_edges(vel_ref, edge_ref):
    tile_height, tile_width = vel_ref.shape[1:]
    edge_ref[...] = jnp.zeros_like(edge_ref)
    for c in range(2):
        edge_ref[4 * c:4 * c + 1, :tile_width] = vel_ref[c, 0:1, :]
        edge_ref[4 * c + 1:4 * c + 2, :tile_width] = vel_ref[c, tile_height - 1:, :]
        turned = jnp.transpose(vel_ref[c])
        edge_ref[4 * c + 2:4 * c + 3, :tile_height] = turned[0:1]
        edge_ref[4 * c + 3:4 * c + 4, :tile_height] = turned[tile_width - 1:]


def sort_particles(aside, owners, width, chunk, part_ref, key_ref, a_ref, b_ref,
                   hot_ref, base_ref, pick_ref, low_ref, acc_ref, sorted_ref, cells_ref, table_ref):
    count = key_ref.shape[1]
    owner_rows = narrow_iota((owners, width), 0)
    ones = jnp.ones((width, LANES), jnp.bfloat16)
    owner_ids = lax.broadcasted_iota(jnp.int32, (owners, LANES), 0)
    tops = count // width

    def count_chunk(index, carry):
        seen, tally = carry
        for part in range(chunk // width):
            start = pl.multiple_of(index * chunk + part * width, width)
            keys = key_ref[:, pl.ds(start, width)]
            hot = one_hot(owner_rows, keys.astype(jnp.float32).astype(jnp.bfloat16))
            hot_ref[:, pl.ds(start, width)] = hot
            base_ref[index * (chunk // width) + part] = seen
            seen = seen + jnp.dot(hot, ones, preferred_element_type=jnp.float32)
            for j in range(width // LANES):
                tally = tally + jnp.where(owner_ids == keys[:, j * LANES:(j + 1) * LANES], 1, 0)
        return seen, tally

    total, tally = lax.fori_loop(0, count // chunk, count_chunk, (
        jnp.zeros((owners, LANES), jnp.float32), jnp.zeros((owners, LANES), jnp.int32)))
    tally = jnp.sum(tally, axis=1, keepdims=True)
    below = (lax.broadcasted_iota(jnp.int32, (owners, owners), 1)
             < lax.broadcasted_iota(jnp.int32, (owners, owners), 0)).astype(jnp.float32).astype(jnp.bfloat16)
    first = jnp.dot(below, total.astype(jnp.bfloat16), preferred_element_type=jnp.float32)
    lane_ids = lax.broadcasted_iota(jnp.int32, (owners, LANES), 1)
    table_ref[0:1, :] = jnp.sum(jnp.where(owner_ids < lane_ids, tally, 0), axis=0, keepdims=True)
    table_ref[1:2, :] = jnp.sum(jnp.where(owner_ids == lane_ids, tally, 0), axis=0, keepdims=True)

    upper = (lax.broadcasted_iota(jnp.int32, (width, width), 0)
             < lax.broadcasted_iota(jnp.int32, (width, width), 1)).astype(jnp.float32).astype(jnp.bfloat16)
    low_rows = narrow_iota((width, width), 0)
    top_rows = narrow_iota((tops, width), 0)
    zero = jnp.zeros((), jnp.bfloat16)

    acc_ref[...] = jnp.zeros_like(acc_ref)

    def place_chunk(index, carry):
        for part in range(chunk // width):
            start = pl.multiple_of(index * chunk + part * width, width)
            at = slice(part * width, (part + 1) * width)
            before = jnp.dot(hot_ref[:, pl.ds(start, width)], upper, preferred_element_type=jnp.float32)
            base = base_ref[index * (chunk // width) + part] + first
            keys = key_ref[:, pl.ds(start, width)]
            spots = []
            for j in range(width // LANES):
                cut = slice(j * LANES, (j + 1) * LANES)
                spots.append(jnp.sum(jnp.where(owner_ids == keys[:, cut], before[:, cut] + base, 0.0),
                                     axis=0, keepdims=True))
            spot = jnp.concatenate(spots, axis=1).astype(jnp.int32)
            top_int = spot // width
            top = top_int.astype(jnp.float32).astype(jnp.bfloat16)
            low = (spot - top_int * width).astype(jnp.float32).astype(jnp.bfloat16)
            low_ref[:, at] = one_hot(low_rows, low)
            values = part_ref[:, pl.ds(start, width)]
            high = rounded(values)
            both = jnp.concatenate([high, values - high], axis=0).astype(jnp.bfloat16)
            for i in range(tops):
                pick_ref[i * 16:(i + 1) * 16, at] = jnp.where(top == jnp.full((), i, jnp.bfloat16), both, zero)
            rows = a_ref[:, pl.ds(start, width)].astype(jnp.float32).astype(jnp.bfloat16)
            cols = b_ref[:, pl.ds(start, width)].astype(jnp.float32).astype(jnp.bfloat16)
            mine = top_rows == top
            pick_ref[tops * 16:tops * 17, at] = jnp.where(mine, rows, zero)
            pick_ref[tops * 17:tops * 18, at] = jnp.where(mine, cols, zero)
        acc_ref[...] += lax.dot_general(pick_ref[...], low_ref[...], NT, preferred_element_type=jnp.float32)
        return carry

    half = count // chunk // 2
    lax.fori_loop(0, half, place_chunk, 0, unroll=2)
    aside()
    lax.fori_loop(half, 2 * half, place_chunk, 0, unroll=2)


def unpack_sorted(tops, width, tile_width, acc_ref, sorted_ref, cells_ref):
    cells = acc_ref[tops * 16:tops * 17, :] * float(tile_width) + acc_ref[tops * 17:tops * 18, :]
    per = width // LANES
    for i in range(tops):
        rows = acc_ref[i * 16:i * 16 + 8, :] + acc_ref[i * 16 + 8:i * 16 + 16, :]
        for j in range(per):
            at = slice(j * LANES, (j + 1) * LANES)
            sorted_ref[i * per + j] = rows[:, at]
            cells_ref[i * per + j, 0:1] = cells[i:i + 1, at]


def cut_block(first, size, sorted_ref, cells_ref, out):
    base = first // LANES
    shift = first - base * LANES
    back = LANES - shift
    lane = lax.broadcasted_iota(jnp.int32, (8, LANES), 1)
    near = lane < back
    turned = [pltpu.roll(sorted_ref[base + j], back, 1) for j in range(3)]
    for j in range(2):
        piece = jnp.where(near, turned[j], turned[j + 1])
        out[8 * j:8 * j + 8, :] = jnp.where(lane + j * LANES < size, piece, 0.0)
    turned = [pltpu.roll(cells_ref[base + j], back, 1) for j in range(3)]
    for j in range(2):
        piece = jnp.where(near, turned[j], turned[j + 1])
        out[16 + j:17 + j, :] = jnp.where(lane + j * LANES < size, piece, -1.0)[0:1]


def build_table(vel_ref, halo_ref, table_ref, tile_height, tile_width):
    width = tile_width + 8
    lane = lax.broadcasted_iota(jnp.int32, (1, LANES), 1)
    tall = tile_height // BLOCK_A
    wide = tile_width // BLOCK_B
    reach = BLOCK_A + 2
    node = lax.broadcasted_iota(jnp.int32, (tile_height + LANES, reach * tall), 0)
    slot = lax.broadcasted_iota(jnp.int32, (tile_height + LANES, reach * tall), 1)
    want = BLOCK_A * (slot % tall) + slot // tall - 1
    want = jnp.where(want < 0, tile_height, jnp.where(want == tile_height, tile_height + 1, want))
    select = (node == want).astype(jnp.float32).astype(jnp.bfloat16)

    def beside(da, db, row):
        return halo_ref[DIRS.index((da, db)), row:row + 1, :]

    largest = jnp.maximum(jnp.max(jnp.abs(vel_ref[0]), axis=0, keepdims=True),
                          jnp.max(jnp.abs(vel_ref[1]), axis=0, keepdims=True))
    border = jnp.max(jnp.abs(halo_ref[0]), axis=0, keepdims=True)
    for k in range(1, 8):
        border = jnp.maximum(border, jnp.max(jnp.abs(halo_ref[k]), axis=0, keepdims=True))
    largest = jnp.maximum(largest, jnp.maximum(border[:, :LANES], border[:, LANES:]))
    largest = jnp.maximum(jnp.max(largest, axis=1, keepdims=True), 1e-30)
    scale = TOP / largest
    extras = [[[] for _ in range(2)] for _ in range(TERMS)]
    for c in range(2):
        own = jnp.transpose(vel_ref[c])
        left = beside(0, -1, 4 * c + 3)[:, :tile_height]
        right = beside(0, 1, 4 * c + 2)[:, :tile_height]
        rest = jnp.zeros((width - tile_width - 2, tile_height), jnp.float32)
        body = jnp.concatenate([own, left, right, rest], axis=0)

        def outer(da, row):
            middle = beside(da, 0, row)[:, :tile_width]
            west = beside(da, -1, row)[:, tile_width - 1:tile_width]
            east = beside(da, 1, row)[:, 0:1]
            return jnp.concatenate(
                [middle, jnp.where(lane == 0, west, jnp.where(lane == 1, east, 0.0))], axis=1)

        ends = jnp.concatenate([outer(-1, 4 * c + 1), outer(1, 4 * c),
                                jnp.zeros((LANES - 2, 2 * LANES), jnp.float32)], axis=0)
        full = jnp.concatenate([body, jnp.transpose(ends)[:width]], axis=1)
        rest, terms = full * scale, []
        for _ in range(TERMS):
            terms.append(rest.astype(NARROW).astype(jnp.float32))
            rest = rest - terms[-1]
        spread = jnp.dot(jnp.concatenate(terms, axis=0).astype(jnp.bfloat16), select,
                         preferred_element_type=jnp.float32)
        first_half = lax.broadcasted_iota(jnp.int32, (BLOCK_B, LANES), 1) < LANES // 2
        for part in range(TERMS):
            z = spread[part * width:(part + 1) * width]
            plain = [z[:, j * LANES:(j + 1) * LANES] for j in range(reach * tall // LANES)]
            turned = [pltpu.roll(p, LANES // 2, 1) for p in plain]

            def joined(i, rows):
                j, half = i // 2, i % 2
                low, top = (plain[j], turned[j]) if half == 0 else (turned[j], plain[j])
                height = rows[0].stop - rows[0].start
                return jnp.concatenate([jnp.where(first_half[:height], low[rows[2 * k]], top[rows[2 * k + 1]])
                                        for k in range(wide // 2)], axis=1)

            columns = slice(part * tall * wide, (part + 1) * tall * wide)
            for i in range(reach):
                low = (c * reach + i) * BLOCK_B
                table_ref[low:low + BLOCK_B, columns] = joined(
                    i, [slice(BLOCK_B * k, BLOCK_B * (k + 1)) for k in range(wide)]).astype(NARROW)
            for e in range(2):
                if e == 0:
                    lines = [tile_width] + [BLOCK_B * k - 1 for k in range(1, wide)]
                else:
                    lines = [BLOCK_B * (k + 1) for k in range(wide - 1)] + [tile_width + 1]
                rows = [joined(i, [slice(r, r + 1) for r in lines]) for i in range(reach)]
                rows.append(jnp.zeros((8 - reach, tall * wide), jnp.float32))
                extras[part][c].append(jnp.concatenate(rows, axis=0))
    for part in range(TERMS):
        columns = slice(part * tall * wide, (part + 1) * tall * wide)
        low = 2 * reach * BLOCK_B
        table_ref[low:low + 32, columns] = jnp.concatenate(extras[part][0] + extras[part][1], axis=0).astype(NARROW)
    return largest * (1.0 / TOP)


def gather_nodes(blocks, tile_width, table_ref, nodes_ref):
    cells = jnp.concatenate([b[16 + j:17 + j, :] for b in blocks for j in range(2)], axis=1)
    cell = jnp.maximum(cells, 0.0).astype(jnp.int32)
    row = cell // tile_width
    col = cell - row * tile_width
    index = (col // BLOCK_B) * 64 + row // BLOCK_A
    index = index.astype(jnp.float32).astype(jnp.bfloat16)
    hot = one_hot(narrow_iota((256, index.shape[1]), 0), index).astype(NARROW)
    nodes_ref[...] = jnp.dot(table_ref[...], jnp.concatenate([hot] * TERMS, axis=0),
                             preferred_element_type=jnp.float32)


def banded(diff, weights):
    return jnp.where(diff == -1, weights[0], jnp.where(diff == 0, weights[1], jnp.where(diff == 1, weights[2], 0.0)))


def weigh(v, cell, tile_width, nodes, step):
    reach = BLOCK_A + 2
    live = cell >= 0.0
    place = jnp.maximum(cell, 0.0).astype(jnp.int32)
    row = place // tile_width
    col = place - row * tile_width
    row = row % BLOCK_A
    col = col % BLOCK_B
    wa = quad_weights(v[0:1])
    wb = quad_weights(v[1:2])
    aw = banded(lax.broadcasted_iota(jnp.int32, (8, LANES), 0) - 1 - row, wa)
    bw = banded(lax.broadcasted_iota(jnp.int32, (BLOCK_B, LANES), 0) - col, wb)
    left = jnp.where(col == 0, wb[0], 0.0)
    right = jnp.where(col == BLOCK_B - 1, wb[2], 0.0)
    scale = jnp.where(live, step, 0.0)
    moved = []
    for c in range(2):
        y = None
        for i in range(reach):
            term = aw[i:i + 1] * nodes(slice((c * reach + i) * BLOCK_B, (c * reach + i + 1) * BLOCK_B))
            y = term if y is None else y + term
        y = y * bw
        low = 2 * reach * BLOCK_B + c * 16
        z = aw * (left * nodes(slice(low, low + 8)) + right * nodes(slice(low + 8, low + 16)))
        for k in range(BLOCK_B // 8):
            z = z + y[8 * k:8 * k + 8]
        moved.append(jnp.sum(z, axis=0, keepdims=True) * scale)
    line = lax.broadcasted_iota(jnp.int32, v.shape, 0)
    return v + jnp.where(line == 2, moved[0], jnp.where(line == 3, moved[1], 0.0))


def advance_block(block, source, at, tile_width, step, nodes_ref, out_ref, cell_ref):
    for j in range(2):
        lanes = slice(at + j * LANES, at + (j + 1) * LANES)
        v = block[8 * j:8 * j + 8, :]
        cell = block[16 + j:17 + j, :]
        out_ref[:, pl.ds(pl.multiple_of(source * 2 * LANES + j * LANES, LANES), LANES)] = weigh(
            v, cell, tile_width, lambda rows, lanes=lanes: nodes_ref[rows, lanes], step)
    cell_ref[pl.ds(source * 2, 2), :] = block[16:18, :].astype(jnp.int32)


def exchange_kernel(sizes, width, chunk, part_ref, key_ref, a_ref, b_ref, vel_ref, out_ref, cell_ref,
                    hot_ref, base_ref, pick_ref, low_ref, acc_ref, sorted_ref, cells_ref, first_ref, first_smem,
                    outgoing, held, edge_ref, halo_ref, table_ref, step_ref, nodes_even, nodes_odd,
                    send_sem, recv_sem, halo_send, halo_recv, local_sem, row_sem):
    nx, ny, nz = sizes
    plane = ny * nz
    n = nx * plane
    group, ahead = 16, 48
    tile_height, tile_width = vel_ref.shape[1:]
    gx, gy, gz = lax.axis_index("gx"), lax.axis_index("gy"), lax.axis_index("gz")
    column = gy * nz + gz

    assert (nx, ny, nz) == (4, 16, 2)

    def at(dx, dyz, sign):
        x = (gx + sign * dx) & (nx - 1)
        y = (gy + sign * (dyz >> 1)) & (ny - 1)
        z = gz ^ (dyz & 1)
        return x, y, z

    def linear(place):
        return (place[0] * ny + place[1]) * nz + place[2]

    def halo_copy(k, slot):
        da, db = DIRS[k]
        there = column + db
        return pltpu.make_async_remote_copy(
            src_ref=edge_ref, dst_ref=halo_ref.at[slot], send_sem=halo_send.at[k],
            recv_sem=halo_recv.at[slot], device_id=(gx + da, there // nz, lax.rem(there, nz)),
            device_id_type=pl.DeviceIdType.MESH)

    def exists(k):
        da, db = DIRS[k]
        a, b = gx + da, column + db
        return (a >= 0) & (a < nx) & (b >= 0) & (b < plane)

    def hop(q):
        core, r = q & 1, q >> 1
        z = r & 3
        x = (r + (r >> 2)) & 3
        y = (r + (r >> 4)) & 3
        return z, (y * 4 + x) * nz + core

    def block_copy(q):
        return pltpu.make_async_remote_copy(
            src_ref=outgoing.at[q], dst_ref=held.at[q],
            send_sem=send_sem, recv_sem=recv_sem.at[(q + group - 2) >> 4], device_id=at(*hop(q), 1),
            device_id_type=pl.DeviceIdType.MESH)

    def arrived(first, size, p):
        some = pl.ds(first, size)
        return pltpu.make_async_remote_copy(
            src_ref=outgoing.at[some], dst_ref=held.at[some], send_sem=send_sem, recv_sem=recv_sem.at[p],
            device_id=at(*hop(1), 1), device_id_type=pl.DeviceIdType.MESH)

    barrier = pltpu.get_barrier_semaphore()

    def row_peer(i):
        return (gx + (i >> 1)) & (nx - 1), gy, gz ^ (i & 1)

    def greet(i, carry):
        pl.semaphore_signal(barrier, inc=1, device_id=(gx, (gy + i) & (ny - 1), gz),
                            device_id_type=pl.DeviceIdType.MESH)
        return carry

    lax.fori_loop(1, ny, greet, 0)
    for i in range(1, nx * nz):
        pl.semaphore_signal(barrier, inc=1, device_id=row_peer(i), device_id_type=pl.DeviceIdType.MESH)

    def pass_on():
        pl.semaphore_wait(barrier, ny - 1 + nx * nz - 1)
        for i in range(1, nx * nz):
            pl.semaphore_signal(row_sem, inc=1, device_id=row_peer(i), device_id_type=pl.DeviceIdType.MESH)

    pack_edges(vel_ref, edge_ref)
    first_ref[...] = jnp.zeros_like(first_ref)
    sort_particles(pass_on, n, width, chunk, part_ref, key_ref, a_ref, b_ref, hot_ref, base_ref, pick_ref,
                   low_ref, acc_ref, sorted_ref, cells_ref, first_ref)
    to_smem = pltpu.make_async_copy(first_ref, first_smem, local_sem)
    to_smem.start()
    tops = key_ref.shape[1] // width
    tail = tops * width // LANES
    sorted_ref[tail:] = jnp.zeros((3, 8, LANES), jnp.float32)
    cells_ref[tail:] = jnp.zeros((3, 8, LANES), jnp.float32)
    unpack_sorted(tops, width, tile_width, acc_ref, sorted_ref, cells_ref)
    to_smem.wait()
    pl.semaphore_wait(row_sem, nx * nz - 1)
    for k in range(8):
        @pl.when(exists(k))
        def _(k=k):
            halo_copy(k, 7 - k).start()

        @pl.when(jnp.logical_not(exists(k)))
        def _(k=k):
            halo_ref[k] = jnp.zeros(halo_ref.shape[1:], jnp.float32)

    def dispatch(p, carry):
        for i in range(8):
            q = p * 8 + i
            owner = linear(at(*hop(q), 1))
            cut_block(first_smem[0, owner], first_smem[1, owner], sorted_ref, cells_ref, outgoing.at[q])

        @pl.when((p > 0) & (p < ahead // 8))
        def _():
            block_copy(p * 8).start()

        @pl.when(p < ahead // 8)
        def _():
            for i in range(1, 8):
                block_copy(p * 8 + i).start()
        return carry

    lax.fori_loop(0, n // 8, dispatch, 0)
    held[0] = outgoing[0]

    for k in range(8):
        @pl.when(exists(k))
        def _(k=k):
            halo_copy(k, k).wait_recv()

    unit = build_table(vel_ref, halo_ref, table_ref, tile_height, tile_width)
    step_ref[...] = jnp.broadcast_to(unit * step_length, step_ref.shape)

    def gather(t, nodes_ref):
        gather_nodes([held.at[2 * t], held.at[2 * t + 1]], tile_width, table_ref, nodes_ref)

    def weigh_pair(t, nodes_ref):
        for i in range(2):
            source = linear(at(*hop(2 * t + i), -1))
            advance_block(held.at[2 * t + i], source, i * 2 * LANES, tile_width, step_ref[0:1, :],
                          nodes_ref, out_ref, cell_ref)

    arrived(1, 1, 0).wait_recv()
    gather(0, nodes_even)

    def one_group(p, carry):
        @pl.when(p < (n - ahead) // 16)
        def _():
            for i in range(16):
                block_copy(ahead + p * 16 + i).start()

        @pl.when(p < n // group - 1)
        def _():
            arrived(p * group + 2, group, p + 1).wait_recv()

        @pl.when(p == n // group - 1)
        def _():
            arrived(n - group + 2, group - 2, n // group).wait_recv()

        first = p * (group // 2)

        for t in range(group // 4):
            gather(first + 2 * t + 1, nodes_odd)
            weigh_pair(first + 2 * t, nodes_even)
            gather(jnp.minimum(first + 2 * t + 2, n // 2 - 1), nodes_even)
            weigh_pair(first + 2 * t + 1, nodes_odd)
        return carry

    lax.fori_loop(0, n // group, one_group, 0)

    arrived(1, n - 1, 0).wait_send()
    for k in range(8):
        @pl.when(exists(k))
        def _(k=k):
            halo_copy(k, 7 - k).wait_send()


def shards(particles, dest_key, cell_a, cell_b, velocity):
    owners = lax.axis_size(("gx", "gy", "gz"))
    count = particles.shape[1]
    cap = 4 * count // owners
    tile_height, tile_width = velocity.shape[1:]
    assert owners == LANES and cap == 2 * LANES and (tile_height, tile_width) == (256, 128)
    width, chunk = 256, 1024
    tops = count // width
    sizes = tuple(lax.axis_size(name) for name in ("gx", "gy", "gz"))
    in_vmem = pl.BlockSpec(memory_space=pltpu.VMEM)
    rows = 12 * BLOCK_B + 32
    binned, binned_cell = pl.pallas_call(
        functools.partial(exchange_kernel, sizes, width, chunk),
        out_shape=(jax.ShapeDtypeStruct((8, owners * cap), jnp.float32),
                   jax.ShapeDtypeStruct((owners * 2, LANES), jnp.int32)),
        in_specs=[in_vmem] * 5,
        out_specs=(in_vmem,) * 2,
        scratch_shapes=[
            pltpu.VMEM((owners, count), jnp.bfloat16),
            pltpu.VMEM((tops, owners, LANES), jnp.float32),
            pltpu.VMEM((tops * 18, chunk), jnp.bfloat16),
            pltpu.VMEM((width, chunk), jnp.bfloat16),
            pltpu.VMEM((tops * 18, width), jnp.float32),
            pltpu.VMEM((count // LANES + 3, 8, LANES), jnp.float32),
            pltpu.VMEM((count // LANES + 3, 8, LANES), jnp.float32),
            pltpu.VMEM((8, LANES), jnp.int32),
            pltpu.SMEM((8, LANES), jnp.int32),
            pltpu.VMEM((owners, 18, LANES), jnp.float32),
            pltpu.VMEM((owners, 18, LANES), jnp.float32),
            pltpu.VMEM((8, max(tile_height, tile_width)), jnp.float32),
            pltpu.VMEM((8, 8, max(tile_height, tile_width)), jnp.float32),
            pltpu.VMEM((rows, TERMS * 256), NARROW),
            pltpu.VMEM((8, LANES), jnp.float32),
            pltpu.VMEM((rows, 4 * LANES), jnp.float32),
            pltpu.VMEM((rows, 4 * LANES), jnp.float32),
            pltpu.SemaphoreType.DMA,
            pltpu.SemaphoreType.DMA((owners // 16 + 1,)),
            pltpu.SemaphoreType.DMA((8,)),
            pltpu.SemaphoreType.DMA((8,)),
            pltpu.SemaphoreType.DMA,
            pltpu.SemaphoreType.REGULAR,
        ],
        compiler_params=pltpu.CompilerParams(collective_id=0, has_side_effects=True),
    )(particles, dest_key.reshape(1, -1), cell_a.reshape(1, -1), cell_b.reshape(1, -1), velocity)
    return (binned, binned_cell.reshape(-1))


def solution(mesh):
    in_specs = (
        P(None, ("gx", "gy", "gz")),
        P(("gx", "gy", "gz")),
        P(("gx", "gy", "gz")),
        P(("gx", "gy", "gz")),
        P(None, "gx", ("gy", "gz")),
    )
    out_specs = (P(None, ("gx", "gy", "gz")), P(("gx", "gy", "gz")))
    return jax.shard_map(shards, mesh=mesh, in_specs=in_specs, out_specs=out_specs, check_vma=False)
```

```python
import functools

import jax
import jax.numpy as jnp
from jax import lax
from jax.experimental import pallas as pl
from jax.experimental.pallas import tpu as pltpu
from jax.sharding import PartitionSpec as P

step_length = 0.5
NT = (((1,), (1,)), ((), ()))
LANES = 128
NARROW = jnp.float8_e4m3fn
TERMS, TOP = 3, 256.0
BLOCK_A, BLOCK_B = 4, 32
DIRS = ((-1, -1), (-1, 0), (-1, 1), (0, -1), (0, 1), (1, -1), (1, 0), (1, 1))


def quad_weights(frac):
    return (0.5 * frac * (frac - 1.0), 1.0 - frac * frac, 0.5 * frac * (frac + 1.0))


def rounded(x):
    return x.astype(jnp.bfloat16).astype(jnp.float32)


def narrow_iota(shape, dim):
    return lax.broadcasted_iota(jnp.int32, shape, dim).astype(jnp.float32).astype(jnp.bfloat16)


def one_hot(row, index):
    one, zero = jnp.ones((), jnp.bfloat16), jnp.zeros((), jnp.bfloat16)
    return jnp.where(row == index, one, zero)


def pack_edges(vel_ref, edge_ref):
    tile_height, tile_width = vel_ref.shape[1:]
    edge_ref[...] = jnp.zeros_like(edge_ref)
    for c in range(2):
        edge_ref[4 * c:4 * c + 1, :tile_width] = vel_ref[c, 0:1, :]
        edge_ref[4 * c + 1:4 * c + 2, :tile_width] = vel_ref[c, tile_height - 1:, :]
        turned = jnp.transpose(vel_ref[c])
        edge_ref[4 * c + 2:4 * c + 3, :tile_height] = turned[0:1]
        edge_ref[4 * c + 3:4 * c + 4, :tile_height] = turned[tile_width - 1:]


def sort_particles(aside, owners, width, chunk, part_ref, key_ref, a_ref, b_ref,
                   hot_ref, base_ref, pick_ref, low_ref, acc_ref, sorted_ref, cells_ref, table_ref):
    count = key_ref.shape[1]
    owner_rows = narrow_iota((owners, width), 0)
    ones = jnp.ones((width, LANES), jnp.bfloat16)
    owner_ids = lax.broadcasted_iota(jnp.int32, (owners, LANES), 0)
    tops = count // width

    def count_chunk(index, carry):
        seen, tally = carry
        for part in range(chunk // width):
            start = pl.multiple_of(index * chunk + part * width, width)
            keys = key_ref[:, pl.ds(start, width)]
            hot = one_hot(owner_rows, keys.astype(jnp.float32).astype(jnp.bfloat16))
            hot_ref[:, pl.ds(start, width)] = hot
            base_ref[index * (chunk // width) + part] = seen
            seen = seen + jnp.dot(hot, ones, preferred_element_type=jnp.float32)
            for j in range(width // LANES):
                tally = tally + jnp.where(owner_ids == keys[:, j * LANES:(j + 1) * LANES], 1, 0)
        return seen, tally

    total, tally = lax.fori_loop(0, count // chunk, count_chunk, (
        jnp.zeros((owners, LANES), jnp.float32), jnp.zeros((owners, LANES), jnp.int32)), unroll=8)
    tally = jnp.sum(tally, axis=1, keepdims=True)
    below = (lax.broadcasted_iota(jnp.int32, (owners, owners), 1)
             < lax.broadcasted_iota(jnp.int32, (owners, owners), 0)).astype(jnp.float32).astype(jnp.bfloat16)
    first = jnp.dot(below, total.astype(jnp.bfloat16), preferred_element_type=jnp.float32)
    lane_ids = lax.broadcasted_iota(jnp.int32, (owners, LANES), 1)
    table_ref[0:1, :] = jnp.sum(jnp.where(owner_ids < lane_ids, tally, 0), axis=0, keepdims=True)
    table_ref[1:2, :] = jnp.sum(jnp.where(owner_ids == lane_ids, tally, 0), axis=0, keepdims=True)

    upper = (lax.broadcasted_iota(jnp.int32, (width, width), 0)
             < lax.broadcasted_iota(jnp.int32, (width, width), 1)).astype(jnp.float32).astype(jnp.bfloat16)
    low_rows = narrow_iota((width, width), 0)
    top_rows = narrow_iota((tops, width), 0)
    zero = jnp.zeros((), jnp.bfloat16)

    acc_ref[...] = jnp.zeros_like(acc_ref)

    def place_chunk(index, carry):
        for part in range(chunk // width):
            start = pl.multiple_of(index * chunk + part * width, width)
            at = slice(part * width, (part + 1) * width)
            before = jnp.dot(hot_ref[:, pl.ds(start, width)], upper, preferred_element_type=jnp.float32)
            base = base_ref[index * (chunk // width) + part] + first
            keys = key_ref[:, pl.ds(start, width)]
            spots = []
            for j in range(width // LANES):
                cut = slice(j * LANES, (j + 1) * LANES)
                spots.append(jnp.sum(jnp.where(owner_ids == keys[:, cut], before[:, cut] + base, 0.0),
                                     axis=0, keepdims=True))
            spot = jnp.concatenate(spots, axis=1).astype(jnp.int32)
            top_int = spot // width
            top = top_int.astype(jnp.float32).astype(jnp.bfloat16)
            low = (spot - top_int * width).astype(jnp.float32).astype(jnp.bfloat16)
            low_ref[:, at] = one_hot(low_rows, low)
            values = part_ref[:, pl.ds(start, width)]
            high = rounded(values)
            both = jnp.concatenate([high, values - high], axis=0).astype(jnp.bfloat16)
            for i in range(tops):
                pick_ref[i * 16:(i + 1) * 16, at] = jnp.where(top == jnp.full((), i, jnp.bfloat16), both, zero)
            rows = a_ref[:, pl.ds(start, width)].astype(jnp.float32).astype(jnp.bfloat16)
            cols = b_ref[:, pl.ds(start, width)].astype(jnp.float32).astype(jnp.bfloat16)
            mine = top_rows == top
            pick_ref[tops * 16:tops * 17, at] = jnp.where(mine, rows, zero)
            pick_ref[tops * 17:tops * 18, at] = jnp.where(mine, cols, zero)
        acc_ref[...] += lax.dot_general(pick_ref[...], low_ref[...], NT, preferred_element_type=jnp.float32)
        return carry

    half = count // chunk // 2
    lax.fori_loop(0, half, place_chunk, 0, unroll=4)
    aside()
    lax.fori_loop(half, 2 * half, place_chunk, 0, unroll=4)


def unpack_sorted(tops, width, tile_width, acc_ref, sorted_ref, cells_ref):
    cells = acc_ref[tops * 16:tops * 17, :] * float(tile_width) + acc_ref[tops * 17:tops * 18, :]
    per = width // LANES
    for i in range(tops):
        rows = acc_ref[i * 16:i * 16 + 8, :] + acc_ref[i * 16 + 8:i * 16 + 16, :]
        for j in range(per):
            at = slice(j * LANES, (j + 1) * LANES)
            sorted_ref[i * per + j] = rows[:, at]
            cells_ref[i * per + j, 0:1] = cells[i:i + 1, at]


def cut_block(first, size, sorted_ref, cells_ref, out):
    base = first // LANES
    shift = first - base * LANES
    back = LANES - shift
    lane = lax.broadcasted_iota(jnp.int32, (8, LANES), 1)
    near = lane < back
    turned = [pltpu.roll(sorted_ref[base + j], back, 1) for j in range(3)]
    for j in range(2):
        piece = jnp.where(near, turned[j], turned[j + 1])
        out[8 * j:8 * j + 8, :] = jnp.where(lane + j * LANES < size, piece, 0.0)
    turned = [pltpu.roll(cells_ref[base + j], back, 1) for j in range(3)]
    for j in range(2):
        piece = jnp.where(near, turned[j], turned[j + 1])
        out[16 + j:17 + j, :] = jnp.where(lane + j * LANES < size, piece, -1.0)[0:1]


def build_table(vel_ref, halo_ref, table_ref, tile_height, tile_width):
    width = tile_width + 8
    lane = lax.broadcasted_iota(jnp.int32, (1, LANES), 1)
    tall = tile_height // BLOCK_A
    wide = tile_width // BLOCK_B
    reach = BLOCK_A + 2
    node = lax.broadcasted_iota(jnp.int32, (tile_height + LANES, reach * tall), 0)
    slot = lax.broadcasted_iota(jnp.int32, (tile_height + LANES, reach * tall), 1)
    want = BLOCK_A * (slot % tall) + slot // tall - 1
    want = jnp.where(want < 0, tile_height, jnp.where(want == tile_height, tile_height + 1, want))
    select = (node == want).astype(jnp.float32).astype(jnp.bfloat16)

    def beside(da, db, row):
        return halo_ref[DIRS.index((da, db)), row:row + 1, :]

    largest = jnp.maximum(jnp.max(jnp.abs(vel_ref[0]), axis=0, keepdims=True),
                          jnp.max(jnp.abs(vel_ref[1]), axis=0, keepdims=True))
    border = jnp.max(jnp.abs(halo_ref[0]), axis=0, keepdims=True)
    for k in range(1, 8):
        border = jnp.maximum(border, jnp.max(jnp.abs(halo_ref[k]), axis=0, keepdims=True))
    largest = jnp.maximum(largest, jnp.maximum(border[:, :LANES], border[:, LANES:]))
    largest = jnp.maximum(jnp.max(largest, axis=1, keepdims=True), 1e-30)
    scale = TOP / largest
    extras = [[[] for _ in range(2)] for _ in range(TERMS)]
    for c in range(2):
        own = jnp.transpose(vel_ref[c])
        left = beside(0, -1, 4 * c + 3)[:, :tile_height]
        right = beside(0, 1, 4 * c + 2)[:, :tile_height]
        rest = jnp.zeros((width - tile_width - 2, tile_height), jnp.float32)
        body = jnp.concatenate([own, left, right, rest], axis=0)

        def outer(da, row):
            middle = beside(da, 0, row)[:, :tile_width]
            west = beside(da, -1, row)[:, tile_width - 1:tile_width]
            east = beside(da, 1, row)[:, 0:1]
            return jnp.concatenate(
                [middle, jnp.where(lane == 0, west, jnp.where(lane == 1, east, 0.0))], axis=1)

        ends = jnp.concatenate([outer(-1, 4 * c + 1), outer(1, 4 * c),
                                jnp.zeros((LANES - 2, 2 * LANES), jnp.float32)], axis=0)
        full = jnp.concatenate([body, jnp.transpose(ends)[:width]], axis=1)
        rest, terms = full * scale, []
        for _ in range(TERMS):
            terms.append(rest.astype(NARROW).astype(jnp.float32))
            rest = rest - terms[-1]
        spread = jnp.dot(jnp.concatenate(terms, axis=0).astype(jnp.bfloat16), select,
                         preferred_element_type=jnp.float32)
        first_half = lax.broadcasted_iota(jnp.int32, (BLOCK_B, LANES), 1) < LANES // 2
        for part in range(TERMS):
            z = spread[part * width:(part + 1) * width]
            plain = [z[:, j * LANES:(j + 1) * LANES] for j in range(reach * tall // LANES)]
            turned = [pltpu.roll(p, LANES // 2, 1) for p in plain]

            def joined(i, rows):
                j, half = i // 2, i % 2
                low, top = (plain[j], turned[j]) if half == 0 else (turned[j], plain[j])
                height = rows[0].stop - rows[0].start
                return jnp.concatenate([jnp.where(first_half[:height], low[rows[2 * k]], top[rows[2 * k + 1]])
                                        for k in range(wide // 2)], axis=1)

            columns = slice(part * tall * wide, (part + 1) * tall * wide)
            for i in range(reach):
                low = (c * reach + i) * BLOCK_B
                table_ref[low:low + BLOCK_B, columns] = joined(
                    i, [slice(BLOCK_B * k, BLOCK_B * (k + 1)) for k in range(wide)]).astype(NARROW)
            for e in range(2):
                if e == 0:
                    lines = [tile_width] + [BLOCK_B * k - 1 for k in range(1, wide)]
                else:
                    lines = [BLOCK_B * (k + 1) for k in range(wide - 1)] + [tile_width + 1]
                rows = [joined(i, [slice(r, r + 1) for r in lines]) for i in range(reach)]
                rows.append(jnp.zeros((8 - reach, tall * wide), jnp.float32))
                extras[part][c].append(jnp.concatenate(rows, axis=0))
    for part in range(TERMS):
        columns = slice(part * tall * wide, (part + 1) * tall * wide)
        low = 2 * reach * BLOCK_B
        table_ref[low:low + 32, columns] = jnp.concatenate(extras[part][0] + extras[part][1], axis=0).astype(NARROW)
    return largest * (1.0 / TOP)


def gather_nodes(blocks, tile_width, table_ref, nodes_ref):
    cells = jnp.concatenate([b[16 + j:17 + j, :] for b in blocks for j in range(2)], axis=1)
    cell = jnp.maximum(cells, 0.0).astype(jnp.int32)
    row = cell // tile_width
    col = cell - row * tile_width
    index = (col // BLOCK_B) * 64 + row // BLOCK_A
    index = index.astype(jnp.float32).astype(jnp.bfloat16)
    hot = one_hot(narrow_iota((256, index.shape[1]), 0), index).astype(NARROW)
    nodes_ref[...] = jnp.dot(table_ref[...], jnp.concatenate([hot] * TERMS, axis=0),
                             preferred_element_type=jnp.float32)


def banded(diff, weights):
    return jnp.where(diff == -1, weights[0], jnp.where(diff == 0, weights[1], jnp.where(diff == 1, weights[2], 0.0)))


def weigh(v, cell, tile_width, nodes, step):
    reach = BLOCK_A + 2
    live = cell >= 0.0
    place = jnp.maximum(cell, 0.0).astype(jnp.int32)
    row = place // tile_width
    col = place - row * tile_width
    row = row % BLOCK_A
    col = col % BLOCK_B
    wa = quad_weights(v[0:1])
    wb = quad_weights(v[1:2])
    aw = banded(lax.broadcasted_iota(jnp.int32, (8, LANES), 0) - 1 - row, wa)
    bw = banded(lax.broadcasted_iota(jnp.int32, (BLOCK_B, LANES), 0) - col, wb)
    left = jnp.where(col == 0, wb[0], 0.0)
    right = jnp.where(col == BLOCK_B - 1, wb[2], 0.0)
    scale = jnp.where(live, step, 0.0)
    moved = []
    for c in range(2):
        y = None
        for i in range(reach):
            term = aw[i:i + 1] * nodes(slice((c * reach + i) * BLOCK_B, (c * reach + i + 1) * BLOCK_B))
            y = term if y is None else y + term
        y = y * bw
        low = 2 * reach * BLOCK_B + c * 16
        z = aw * (left * nodes(slice(low, low + 8)) + right * nodes(slice(low + 8, low + 16)))
        for k in range(BLOCK_B // 8):
            z = z + y[8 * k:8 * k + 8]
        moved.append(jnp.sum(z, axis=0, keepdims=True) * scale)
    line = lax.broadcasted_iota(jnp.int32, v.shape, 0)
    return v + jnp.where(line == 2, moved[0], jnp.where(line == 3, moved[1], 0.0))


def advance_block(block, source, at, tile_width, step, nodes_ref, out_ref, cell_ref):
    for j in range(2):
        lanes = slice(at + j * LANES, at + (j + 1) * LANES)
        v = block[8 * j:8 * j + 8, :]
        cell = block[16 + j:17 + j, :]
        out_ref[:, pl.ds(pl.multiple_of(source * 2 * LANES + j * LANES, LANES), LANES)] = weigh(
            v, cell, tile_width, lambda rows, lanes=lanes: nodes_ref[rows, lanes], step)
    cell_ref[pl.ds(source * 2, 2), :] = block[16:18, :].astype(jnp.int32)


def exchange_kernel(sizes, width, chunk, part_ref, key_ref, a_ref, b_ref, vel_ref, out_ref, cell_ref,
                    hot_ref, base_ref, pick_ref, low_ref, acc_ref, sorted_ref, cells_ref, first_ref, first_smem,
                    outgoing, held, edge_ref, halo_ref, table_ref, step_ref, nodes_even, nodes_odd,
                    send_sem, recv_sem, halo_send, halo_recv, local_sem, row_sem):
    nx, ny, nz = sizes
    plane = ny * nz
    n = nx * plane
    group, ahead = 16, 48
    tile_height, tile_width = vel_ref.shape[1:]
    gx, gy, gz = lax.axis_index("gx"), lax.axis_index("gy"), lax.axis_index("gz")
    column = gy * nz + gz

    assert (nx, ny, nz) == (4, 16, 2)

    def at(dx, dyz, sign):
        x = (gx + sign * dx) & (nx - 1)
        y = (gy + sign * (dyz >> 1)) & (ny - 1)
        z = gz ^ (dyz & 1)
        return x, y, z

    def linear(place):
        return (place[0] * ny + place[1]) * nz + place[2]

    def halo_copy(k, slot):
        da, db = DIRS[k]
        there = column + db
        return pltpu.make_async_remote_copy(
            src_ref=edge_ref, dst_ref=halo_ref.at[slot], send_sem=halo_send.at[k],
            recv_sem=halo_recv.at[slot], device_id=(gx + da, there // nz, lax.rem(there, nz)),
            device_id_type=pl.DeviceIdType.MESH)

    def exists(k):
        da, db = DIRS[k]
        a, b = gx + da, column + db
        return (a >= 0) & (a < nx) & (b >= 0) & (b < plane)

    def hop(q):
        core, r = q & 1, q >> 1
        z = r & 3
        x = (r + (r >> 2)) & 3
        y = (r + (r >> 4)) & 3
        return z, (y * 4 + x) * nz + core

    def block_copy(q):
        return pltpu.make_async_remote_copy(
            src_ref=outgoing.at[q], dst_ref=held.at[q],
            send_sem=send_sem, recv_sem=recv_sem.at[(q + group - 2) >> 4], device_id=at(*hop(q), 1),
            device_id_type=pl.DeviceIdType.MESH)

    def arrived(first, size, p):
        some = pl.ds(first, size)
        return pltpu.make_async_remote_copy(
            src_ref=outgoing.at[some], dst_ref=held.at[some], send_sem=send_sem, recv_sem=recv_sem.at[p],
            device_id=at(*hop(1), 1), device_id_type=pl.DeviceIdType.MESH)

    barrier = pltpu.get_barrier_semaphore()

    def row_peer(i):
        return (gx + (i >> 1)) & (nx - 1), gy, gz ^ (i & 1)

    def greet(i, carry):
        pl.semaphore_signal(barrier, inc=1, device_id=(gx, (gy + i) & (ny - 1), gz),
                            device_id_type=pl.DeviceIdType.MESH)
        return carry

    lax.fori_loop(1, ny, greet, 0)
    for i in range(1, nx * nz):
        pl.semaphore_signal(barrier, inc=1, device_id=row_peer(i), device_id_type=pl.DeviceIdType.MESH)

    def pass_on():
        pl.semaphore_wait(barrier, ny - 1 + nx * nz - 1)
        for i in range(1, nx * nz):
            pl.semaphore_signal(row_sem, inc=1, device_id=row_peer(i), device_id_type=pl.DeviceIdType.MESH)

    pack_edges(vel_ref, edge_ref)
    first_ref[...] = jnp.zeros_like(first_ref)
    sort_particles(pass_on, n, width, chunk, part_ref, key_ref, a_ref, b_ref, hot_ref, base_ref, pick_ref,
                   low_ref, acc_ref, sorted_ref, cells_ref, first_ref)
    to_smem = pltpu.make_async_copy(first_ref, first_smem, local_sem)
    to_smem.start()
    tops = key_ref.shape[1] // width
    tail = tops * width // LANES
    sorted_ref[tail:] = jnp.zeros((3, 8, LANES), jnp.float32)
    cells_ref[tail:] = jnp.zeros((3, 8, LANES), jnp.float32)
    unpack_sorted(tops, width, tile_width, acc_ref, sorted_ref, cells_ref)
    to_smem.wait()
    pl.semaphore_wait(row_sem, nx * nz - 1)
    for k in range(8):
        @pl.when(exists(k))
        def _(k=k):
            halo_copy(k, 7 - k).start()

        @pl.when(jnp.logical_not(exists(k)))
        def _(k=k):
            halo_ref[k] = jnp.zeros(halo_ref.shape[1:], jnp.float32)

    def dispatch(p, carry):
        for i in range(16):
            q = p * 16 + i
            owner = linear(at(*hop(q), 1))
            cut_block(first_smem[0, owner], first_smem[1, owner], sorted_ref, cells_ref, outgoing.at[q])

        @pl.when((p > 0) & (p < ahead // 16))
        def _():
            block_copy(p * 16).start()

        @pl.when(p < ahead // 16)
        def _():
            for i in range(1, 16):
                block_copy(p * 16 + i).start()
        return carry

    lax.fori_loop(0, n // 16, dispatch, 0)
    held[0] = outgoing[0]

    for k in range(8):
        @pl.when(exists(k))
        def _(k=k):
            halo_copy(k, k).wait_recv()

    unit = build_table(vel_ref, halo_ref, table_ref, tile_height, tile_width)
    step_ref[...] = jnp.broadcast_to(unit * step_length, step_ref.shape)

    def gather(t, nodes_ref):
        gather_nodes([held.at[2 * t], held.at[2 * t + 1]], tile_width, table_ref, nodes_ref)

    def weigh_pair(t, nodes_ref):
        for i in range(2):
            source = linear(at(*hop(2 * t + i), -1))
            advance_block(held.at[2 * t + i], source, i * 2 * LANES, tile_width, step_ref[0:1, :],
                          nodes_ref, out_ref, cell_ref)

    arrived(1, 1, 0).wait_recv()
    gather(0, nodes_even)

    def one_group(p, carry):
        @pl.when(p < (n - ahead) // 16)
        def _():
            for i in range(16):
                block_copy(ahead + p * 16 + i).start()

        @pl.when(p < n // group - 1)
        def _():
            arrived(p * group + 2, group, p + 1).wait_recv()

        @pl.when(p == n // group - 1)
        def _():
            arrived(n - group + 2, group - 2, n // group).wait_recv()

        first = p * (group // 2)

        for t in range(group // 4):
            gather(first + 2 * t + 1, nodes_odd)
            weigh_pair(first + 2 * t, nodes_even)
            gather(jnp.minimum(first + 2 * t + 2, n // 2 - 1), nodes_even)
            weigh_pair(first + 2 * t + 1, nodes_odd)
        return carry

    lax.fori_loop(0, n // group, one_group, 0)

    arrived(1, n - 1, 0).wait_send()
    for k in range(8):
        @pl.when(exists(k))
        def _(k=k):
            halo_copy(k, 7 - k).wait_send()


def shards(particles, dest_key, cell_a, cell_b, velocity):
    owners = lax.axis_size(("gx", "gy", "gz"))
    count = particles.shape[1]
    cap = 4 * count // owners
    tile_height, tile_width = velocity.shape[1:]
    assert owners == LANES and cap == 2 * LANES and (tile_height, tile_width) == (256, 128)
    width, chunk = 256, 1024
    tops = count // width
    sizes = tuple(lax.axis_size(name) for name in ("gx", "gy", "gz"))
    in_vmem = pl.BlockSpec(memory_space=pltpu.VMEM)
    rows = 12 * BLOCK_B + 32
    binned, binned_cell = pl.pallas_call(
        functools.partial(exchange_kernel, sizes, width, chunk),
        out_shape=(jax.ShapeDtypeStruct((8, owners * cap), jnp.float32),
                   jax.ShapeDtypeStruct((owners * 2, LANES), jnp.int32)),
        in_specs=[in_vmem] * 5,
        out_specs=(in_vmem,) * 2,
        scratch_shapes=[
            pltpu.VMEM((owners, count), jnp.bfloat16),
            pltpu.VMEM((tops, owners, LANES), jnp.float32),
            pltpu.VMEM((tops * 18, chunk), jnp.bfloat16),
            pltpu.VMEM((width, chunk), jnp.bfloat16),
            pltpu.VMEM((tops * 18, width), jnp.float32),
            pltpu.VMEM((count // LANES + 3, 8, LANES), jnp.float32),
            pltpu.VMEM((count // LANES + 3, 8, LANES), jnp.float32),
            pltpu.VMEM((8, LANES), jnp.int32),
            pltpu.SMEM((8, LANES), jnp.int32),
            pltpu.VMEM((owners, 18, LANES), jnp.float32),
            pltpu.VMEM((owners, 18, LANES), jnp.float32),
            pltpu.VMEM((8, max(tile_height, tile_width)), jnp.float32),
            pltpu.VMEM((8, 8, max(tile_height, tile_width)), jnp.float32),
            pltpu.VMEM((rows, TERMS * 256), NARROW),
            pltpu.VMEM((8, LANES), jnp.float32),
            pltpu.VMEM((rows, 4 * LANES), jnp.float32),
            pltpu.VMEM((rows, 4 * LANES), jnp.float32),
            pltpu.SemaphoreType.DMA,
            pltpu.SemaphoreType.DMA((owners // 16 + 1,)),
            pltpu.SemaphoreType.DMA((8,)),
            pltpu.SemaphoreType.DMA((8,)),
            pltpu.SemaphoreType.DMA,
            pltpu.SemaphoreType.REGULAR,
        ],
        compiler_params=pltpu.CompilerParams(collective_id=0, has_side_effects=True),
    )(particles, dest_key.reshape(1, -1), cell_a.reshape(1, -1), cell_b.reshape(1, -1), velocity)
    return (binned, binned_cell.reshape(-1))


def solution(mesh):
    in_specs = (
        P(None, ("gx", "gy", "gz")),
        P(("gx", "gy", "gz")),
        P(("gx", "gy", "gz")),
        P(("gx", "gy", "gz")),
        P(None, "gx", ("gy", "gz")),
    )
    out_specs = (P(None, ("gx", "gy", "gz")), P(("gx", "gy", "gz")))
    return jax.shard_map(shards, mesh=mesh, in_specs=in_specs, out_specs=out_specs, check_vma=False)
```

```python
import functools

import jax
import jax.numpy as jnp
from jax import lax
from jax.experimental import pallas as pl
from jax.experimental.pallas import tpu as pltpu
from jax.sharding import PartitionSpec as P

step_length = 0.5
NT = (((1,), (1,)), ((), ()))
LANES = 128
NARROW = jnp.float8_e4m3fn
TERMS, TOP = 3, 256.0
BLOCK_A, BLOCK_B = 4, 32
DIRS = ((-1, -1), (-1, 0), (-1, 1), (0, -1), (0, 1), (1, -1), (1, 0), (1, 1))


def quad_weights(frac):
    return (0.5 * frac * (frac - 1.0), 1.0 - frac * frac, 0.5 * frac * (frac + 1.0))


def rounded(x):
    return x.astype(jnp.bfloat16).astype(jnp.float32)


def narrow_iota(shape, dim):
    return lax.broadcasted_iota(jnp.int32, shape, dim).astype(jnp.float32).astype(jnp.bfloat16)


def one_hot(row, index):
    one, zero = jnp.ones((), jnp.bfloat16), jnp.zeros((), jnp.bfloat16)
    return jnp.where(row == index, one, zero)


def pack_edges(vel_ref, edge_ref):
    tile_height, tile_width = vel_ref.shape[1:]
    edge_ref[...] = jnp.zeros_like(edge_ref)
    for c in range(2):
        edge_ref[4 * c:4 * c + 1, :tile_width] = vel_ref[c, 0:1, :]
        edge_ref[4 * c + 1:4 * c + 2, :tile_width] = vel_ref[c, tile_height - 1:, :]
        turned = jnp.transpose(vel_ref[c])
        edge_ref[4 * c + 2:4 * c + 3, :tile_height] = turned[0:1]
        edge_ref[4 * c + 3:4 * c + 4, :tile_height] = turned[tile_width - 1:]


def sort_particles(aside, owners, width, chunk, part_ref, key_ref, a_ref, b_ref,
                   hot_ref, base_ref, pick_ref, low_ref, acc_ref, sorted_ref, cells_ref, table_ref):
    count = key_ref.shape[1]
    owner_rows = narrow_iota((owners, width), 0)
    ones = jnp.ones((width, LANES), jnp.bfloat16)
    owner_ids = lax.broadcasted_iota(jnp.int32, (owners, LANES), 0)
    tops = count // width

    def count_chunk(index, carry):
        seen, tally = carry
        for part in range(chunk // width):
            start = pl.multiple_of(index * chunk + part * width, width)
            keys = key_ref[:, pl.ds(start, width)]
            hot = one_hot(owner_rows, keys.astype(jnp.float32).astype(jnp.bfloat16))
            hot_ref[:, pl.ds(start, width)] = hot
            base_ref[index * (chunk // width) + part] = seen
            seen = seen + jnp.dot(hot, ones, preferred_element_type=jnp.float32)
            for j in range(width // LANES):
                tally = tally + jnp.where(owner_ids == keys[:, j * LANES:(j + 1) * LANES], 1, 0)
        return seen, tally

    total, tally = lax.fori_loop(0, count // chunk, count_chunk, (
        jnp.zeros((owners, LANES), jnp.float32), jnp.zeros((owners, LANES), jnp.int32)), unroll=8)
    tally = jnp.sum(tally, axis=1, keepdims=True)
    below = (lax.broadcasted_iota(jnp.int32, (owners, owners), 1)
             < lax.broadcasted_iota(jnp.int32, (owners, owners), 0)).astype(jnp.float32).astype(jnp.bfloat16)
    first = jnp.dot(below, total.astype(jnp.bfloat16), preferred_element_type=jnp.float32)
    lane_ids = lax.broadcasted_iota(jnp.int32, (owners, LANES), 1)
    table_ref[0:1, :] = jnp.sum(jnp.where(owner_ids < lane_ids, tally, 0), axis=0, keepdims=True)
    table_ref[1:2, :] = jnp.sum(jnp.where(owner_ids == lane_ids, tally, 0), axis=0, keepdims=True)

    upper = (lax.broadcasted_iota(jnp.int32, (width, width), 0)
             < lax.broadcasted_iota(jnp.int32, (width, width), 1)).astype(jnp.float32).astype(jnp.bfloat16)
    low_rows = narrow_iota((width, width), 0)
    top_rows = narrow_iota((tops, width), 0)
    zero = jnp.zeros((), jnp.bfloat16)

    acc_ref[...] = jnp.zeros_like(acc_ref)

    def place_chunk(index, carry):
        for part in range(chunk // width):
            start = pl.multiple_of(index * chunk + part * width, width)
            at = slice(part * width, (part + 1) * width)
            before = jnp.dot(hot_ref[:, pl.ds(start, width)], upper, preferred_element_type=jnp.float32)
            base = base_ref[index * (chunk // width) + part] + first
            keys = key_ref[:, pl.ds(start, width)]
            spots = []
            for j in range(width // LANES):
                cut = slice(j * LANES, (j + 1) * LANES)
                spots.append(jnp.sum(jnp.where(owner_ids == keys[:, cut], before[:, cut] + base, 0.0),
                                     axis=0, keepdims=True))
            spot = jnp.concatenate(spots, axis=1).astype(jnp.int32)
            top_int = spot // width
            top = top_int.astype(jnp.float32).astype(jnp.bfloat16)
            low = (spot - top_int * width).astype(jnp.float32).astype(jnp.bfloat16)
            low_ref[:, at] = one_hot(low_rows, low)
            values = part_ref[:, pl.ds(start, width)]
            high = rounded(values)
            both = jnp.concatenate([high, values - high], axis=0).astype(jnp.bfloat16)
            for i in range(tops):
                pick_ref[i * 16:(i + 1) * 16, at] = jnp.where(top == jnp.full((), i, jnp.bfloat16), both, zero)
            rows = a_ref[:, pl.ds(start, width)].astype(jnp.float32).astype(jnp.bfloat16)
            cols = b_ref[:, pl.ds(start, width)].astype(jnp.float32).astype(jnp.bfloat16)
            mine = top_rows == top
            pick_ref[tops * 16:tops * 17, at] = jnp.where(mine, rows, zero)
            pick_ref[tops * 17:tops * 18, at] = jnp.where(mine, cols, zero)
        acc_ref[...] += lax.dot_general(pick_ref[...], low_ref[...], NT, preferred_element_type=jnp.float32)
        return carry

    turn = 6
    lax.fori_loop(0, turn, place_chunk, 0, unroll=6)
    aside()
    lax.fori_loop(turn, count // chunk, place_chunk, 0, unroll=2)


def unpack_sorted(tops, width, tile_width, acc_ref, sorted_ref, cells_ref):
    cells = acc_ref[tops * 16:tops * 17, :] * float(tile_width) + acc_ref[tops * 17:tops * 18, :]
    per = width // LANES
    for i in range(tops):
        rows = acc_ref[i * 16:i * 16 + 8, :] + acc_ref[i * 16 + 8:i * 16 + 16, :]
        for j in range(per):
            at = slice(j * LANES, (j + 1) * LANES)
            sorted_ref[i * per + j] = rows[:, at]
            cells_ref[i * per + j, 0:1] = cells[i:i + 1, at]


def cut_block(first, size, sorted_ref, cells_ref, out):
    base = first // LANES
    shift = first - base * LANES
    back = LANES - shift
    lane = lax.broadcasted_iota(jnp.int32, (8, LANES), 1)
    near = lane < back
    turned = [pltpu.roll(sorted_ref[base + j], back, 1) for j in range(3)]
    for j in range(2):
        piece = jnp.where(near, turned[j], turned[j + 1])
        out[8 * j:8 * j + 8, :] = jnp.where(lane + j * LANES < size, piece, 0.0)
    turned = [pltpu.roll(cells_ref[base + j], back, 1) for j in range(3)]
    for j in range(2):
        piece = jnp.where(near, turned[j], turned[j + 1])
        out[16 + j:17 + j, :] = jnp.where(lane + j * LANES < size, piece, -1.0)[0:1]


def build_table(vel_ref, halo_ref, table_ref, tile_height, tile_width):
    width = tile_width + 8
    lane = lax.broadcasted_iota(jnp.int32, (1, LANES), 1)
    tall = tile_height // BLOCK_A
    wide = tile_width // BLOCK_B
    reach = BLOCK_A + 2
    node = lax.broadcasted_iota(jnp.int32, (tile_height + LANES, reach * tall), 0)
    slot = lax.broadcasted_iota(jnp.int32, (tile_height + LANES, reach * tall), 1)
    want = BLOCK_A * (slot % tall) + slot // tall - 1
    want = jnp.where(want < 0, tile_height, jnp.where(want == tile_height, tile_height + 1, want))
    select = (node == want).astype(jnp.float32).astype(jnp.bfloat16)

    def beside(da, db, row):
        return halo_ref[DIRS.index((da, db)), row:row + 1, :]

    largest = jnp.maximum(jnp.max(jnp.abs(vel_ref[0]), axis=0, keepdims=True),
                          jnp.max(jnp.abs(vel_ref[1]), axis=0, keepdims=True))
    border = jnp.max(jnp.abs(halo_ref[0]), axis=0, keepdims=True)
    for k in range(1, 8):
        border = jnp.maximum(border, jnp.max(jnp.abs(halo_ref[k]), axis=0, keepdims=True))
    largest = jnp.maximum(largest, jnp.maximum(border[:, :LANES], border[:, LANES:]))
    largest = jnp.maximum(jnp.max(largest, axis=1, keepdims=True), 1e-30)
    scale = TOP / largest
    extras = [[[] for _ in range(2)] for _ in range(TERMS)]
    for c in range(2):
        own = jnp.transpose(vel_ref[c])
        left = beside(0, -1, 4 * c + 3)[:, :tile_height]
        right = beside(0, 1, 4 * c + 2)[:, :tile_height]
        rest = jnp.zeros((width - tile_width - 2, tile_height), jnp.float32)
        body = jnp.concatenate([own, left, right, rest], axis=0)

        def outer(da, row):
            middle = beside(da, 0, row)[:, :tile_width]
            west = beside(da, -1, row)[:, tile_width - 1:tile_width]
            east = beside(da, 1, row)[:, 0:1]
            return jnp.concatenate(
                [middle, jnp.where(lane == 0, west, jnp.where(lane == 1, east, 0.0))], axis=1)

        ends = jnp.concatenate([outer(-1, 4 * c + 1), outer(1, 4 * c),
                                jnp.zeros((LANES - 2, 2 * LANES), jnp.float32)], axis=0)
        full = jnp.concatenate([body, jnp.transpose(ends)[:width]], axis=1)
        rest, terms = full * scale, []
        for _ in range(TERMS):
            terms.append(rest.astype(NARROW).astype(jnp.float32))
            rest = rest - terms[-1]
        spread = jnp.dot(jnp.concatenate(terms, axis=0).astype(jnp.bfloat16), select,
                         preferred_element_type=jnp.float32)
        first_half = lax.broadcasted_iota(jnp.int32, (BLOCK_B, LANES), 1) < LANES // 2
        for part in range(TERMS):
            z = spread[part * width:(part + 1) * width]
            plain = [z[:, j * LANES:(j + 1) * LANES] for j in range(reach * tall // LANES)]
            turned = [pltpu.roll(p, LANES // 2, 1) for p in plain]

            def joined(i, rows):
                j, half = i // 2, i % 2
                low, top = (plain[j], turned[j]) if half == 0 else (turned[j], plain[j])
                height = rows[0].stop - rows[0].start
                return jnp.concatenate([jnp.where(first_half[:height], low[rows[2 * k]], top[rows[2 * k + 1]])
                                        for k in range(wide // 2)], axis=1)

            columns = slice(part * tall * wide, (part + 1) * tall * wide)
            for i in range(reach):
                low = (c * reach + i) * BLOCK_B
                table_ref[low:low + BLOCK_B, columns] = joined(
                    i, [slice(BLOCK_B * k, BLOCK_B * (k + 1)) for k in range(wide)]).astype(NARROW)
            for e in range(2):
                if e == 0:
                    lines = [tile_width] + [BLOCK_B * k - 1 for k in range(1, wide)]
                else:
                    lines = [BLOCK_B * (k + 1) for k in range(wide - 1)] + [tile_width + 1]
                rows = [joined(i, [slice(r, r + 1) for r in lines]) for i in range(reach)]
                rows.append(jnp.zeros((8 - reach, tall * wide), jnp.float32))
                extras[part][c].append(jnp.concatenate(rows, axis=0))
    for part in range(TERMS):
        columns = slice(part * tall * wide, (part + 1) * tall * wide)
        low = 2 * reach * BLOCK_B
        table_ref[low:low + 32, columns] = jnp.concatenate(extras[part][0] + extras[part][1], axis=0).astype(NARROW)
    return largest * (1.0 / TOP)


def gather_nodes(blocks, tile_width, table_ref, nodes_ref):
    cells = jnp.concatenate([b[16 + j:17 + j, :] for b in blocks for j in range(2)], axis=1)
    cell = jnp.maximum(cells, 0.0).astype(jnp.int32)
    row = cell // tile_width
    col = cell - row * tile_width
    index = (col // BLOCK_B) * 64 + row // BLOCK_A
    index = index.astype(jnp.float32).astype(jnp.bfloat16)
    hot = one_hot(narrow_iota((256, index.shape[1]), 0), index).astype(NARROW)
    nodes_ref[...] = jnp.dot(table_ref[...], jnp.concatenate([hot] * TERMS, axis=0),
                             preferred_element_type=jnp.float32)


def banded(diff, weights):
    return jnp.where(diff == -1, weights[0], jnp.where(diff == 0, weights[1], jnp.where(diff == 1, weights[2], 0.0)))


def weigh(v, cell, tile_width, nodes, step):
    reach = BLOCK_A + 2
    live = cell >= 0.0
    place = jnp.maximum(cell, 0.0).astype(jnp.int32)
    row = place // tile_width
    col = place - row * tile_width
    row = row % BLOCK_A
    col = col % BLOCK_B
    wa = quad_weights(v[0:1])
    wb = quad_weights(v[1:2])
    aw = banded(lax.broadcasted_iota(jnp.int32, (8, LANES), 0) - 1 - row, wa)
    bw = banded(lax.broadcasted_iota(jnp.int32, (BLOCK_B, LANES), 0) - col, wb)
    left = jnp.where(col == 0, wb[0], 0.0)
    right = jnp.where(col == BLOCK_B - 1, wb[2], 0.0)
    scale = jnp.where(live, step, 0.0)
    moved = []
    for c in range(2):
        y = None
        for i in range(reach):
            term = aw[i:i + 1] * nodes(slice((c * reach + i) * BLOCK_B, (c * reach + i + 1) * BLOCK_B))
            y = term if y is None else y + term
        y = y * bw
        low = 2 * reach * BLOCK_B + c * 16
        z = aw * (left * nodes(slice(low, low + 8)) + right * nodes(slice(low + 8, low + 16)))
        for k in range(BLOCK_B // 8):
            z = z + y[8 * k:8 * k + 8]
        moved.append(jnp.sum(z, axis=0, keepdims=True) * scale)
    line = lax.broadcasted_iota(jnp.int32, v.shape, 0)
    return v + jnp.where(line == 2, moved[0], jnp.where(line == 3, moved[1], 0.0))


def advance_block(block, source, at, tile_width, step, nodes_ref, out_ref, cell_ref):
    for j in range(2):
        lanes = slice(at + j * LANES, at + (j + 1) * LANES)
        v = block[8 * j:8 * j + 8, :]
        cell = block[16 + j:17 + j, :]
        out_ref[:, pl.ds(pl.multiple_of(source * 2 * LANES + j * LANES, LANES), LANES)] = weigh(
            v, cell, tile_width, lambda rows, lanes=lanes: nodes_ref[rows, lanes], step)
    cell_ref[pl.ds(source * 2, 2), :] = block[16:18, :].astype(jnp.int32)


def exchange_kernel(sizes, width, chunk, part_ref, key_ref, a_ref, b_ref, vel_ref, out_ref, cell_ref,
                    hot_ref, base_ref, pick_ref, low_ref, acc_ref, sorted_ref, cells_ref, first_ref, first_smem,
                    outgoing, held, edge_ref, halo_ref, table_ref, step_ref, nodes_even, nodes_odd,
                    send_sem, recv_sem, halo_send, halo_recv, local_sem, row_sem):
    nx, ny, nz = sizes
    plane = ny * nz
    n = nx * plane
    group, ahead = 16, 48
    tile_height, tile_width = vel_ref.shape[1:]
    gx, gy, gz = lax.axis_index("gx"), lax.axis_index("gy"), lax.axis_index("gz")
    column = gy * nz + gz

    assert (nx, ny, nz) == (4, 16, 2)

    def at(dx, dyz, sign):
        x = (gx + sign * dx) & (nx - 1)
        y = (gy + sign * (dyz >> 1)) & (ny - 1)
        z = gz ^ (dyz & 1)
        return x, y, z

    def linear(place):
        return (place[0] * ny + place[1]) * nz + place[2]

    def halo_copy(k, slot):
        da, db = DIRS[k]
        there = column + db
        return pltpu.make_async_remote_copy(
            src_ref=edge_ref, dst_ref=halo_ref.at[slot], send_sem=halo_send.at[k],
            recv_sem=halo_recv.at[slot], device_id=(gx + da, there // nz, lax.rem(there, nz)),
            device_id_type=pl.DeviceIdType.MESH)

    def exists(k):
        da, db = DIRS[k]
        a, b = gx + da, column + db
        return (a >= 0) & (a < nx) & (b >= 0) & (b < plane)

    def hop(q):
        core, r = q & 1, q >> 1
        z = r & 3
        x = (r + (r >> 2)) & 3
        y = (r + (r >> 4)) & 3
        return z, (y * 4 + x) * nz + core

    def block_copy(q):
        return pltpu.make_async_remote_copy(
            src_ref=outgoing.at[q], dst_ref=held.at[q],
            send_sem=send_sem, recv_sem=recv_sem.at[(q + group - 2) >> 4], device_id=at(*hop(q), 1),
            device_id_type=pl.DeviceIdType.MESH)

    def arrived(first, size, p):
        some = pl.ds(first, size)
        return pltpu.make_async_remote_copy(
            src_ref=outgoing.at[some], dst_ref=held.at[some], send_sem=send_sem, recv_sem=recv_sem.at[p],
            device_id=at(*hop(1), 1), device_id_type=pl.DeviceIdType.MESH)

    barrier = pltpu.get_barrier_semaphore()

    def row_peer(i):
        return (gx + (i >> 1)) & (nx - 1), gy, gz ^ (i & 1)

    def greet(i, carry):
        pl.semaphore_signal(barrier, inc=1, device_id=(gx, (gy + i) & (ny - 1), gz),
                            device_id_type=pl.DeviceIdType.MESH)
        return carry

    lax.fori_loop(1, ny, greet, 0)
    for i in range(1, nx * nz):
        pl.semaphore_signal(barrier, inc=1, device_id=row_peer(i), device_id_type=pl.DeviceIdType.MESH)

    def pass_on():
        pl.semaphore_wait(barrier, ny - 1 + nx * nz - 1)
        for i in range(1, nx * nz):
            pl.semaphore_signal(row_sem, inc=1, device_id=row_peer(i), device_id_type=pl.DeviceIdType.MESH)

    pack_edges(vel_ref, edge_ref)
    first_ref[...] = jnp.zeros_like(first_ref)
    sort_particles(pass_on, n, width, chunk, part_ref, key_ref, a_ref, b_ref, hot_ref, base_ref, pick_ref,
                   low_ref, acc_ref, sorted_ref, cells_ref, first_ref)
    to_smem = pltpu.make_async_copy(first_ref, first_smem, local_sem)
    to_smem.start()
    tops = key_ref.shape[1] // width
    tail = tops * width // LANES
    sorted_ref[tail:] = jnp.zeros((3, 8, LANES), jnp.float32)
    cells_ref[tail:] = jnp.zeros((3, 8, LANES), jnp.float32)
    unpack_sorted(tops, width, tile_width, acc_ref, sorted_ref, cells_ref)
    to_smem.wait()
    pl.semaphore_wait(row_sem, nx * nz - 1)
    for k in range(8):
        @pl.when(exists(k))
        def _(k=k):
            halo_copy(k, 7 - k).start()

        @pl.when(jnp.logical_not(exists(k)))
        def _(k=k):
            halo_ref[k] = jnp.zeros(halo_ref.shape[1:], jnp.float32)

    def dispatch(p, carry):
        for i in range(16):
            q = p * 16 + i
            owner = linear(at(*hop(q), 1))
            cut_block(first_smem[0, owner], first_smem[1, owner], sorted_ref, cells_ref, outgoing.at[q])

        @pl.when((p > 0) & (p < ahead // 16))
        def _():
            block_copy(p * 16).start()

        @pl.when(p < ahead // 16)
        def _():
            for i in range(1, 16):
                block_copy(p * 16 + i).start()
        return carry

    lax.fori_loop(0, n // 16, dispatch, 0)
    held[0] = outgoing[0]

    for k in range(8):
        @pl.when(exists(k))
        def _(k=k):
            halo_copy(k, k).wait_recv()

    unit = build_table(vel_ref, halo_ref, table_ref, tile_height, tile_width)
    step_ref[...] = jnp.broadcast_to(unit * step_length, step_ref.shape)

    def gather(t, nodes_ref):
        gather_nodes([held.at[2 * t], held.at[2 * t + 1]], tile_width, table_ref, nodes_ref)

    def weigh_pair(t, nodes_ref):
        for i in range(2):
            source = linear(at(*hop(2 * t + i), -1))
            advance_block(held.at[2 * t + i], source, i * 2 * LANES, tile_width, step_ref[0:1, :],
                          nodes_ref, out_ref, cell_ref)

    arrived(1, 1, 0).wait_recv()
    gather(0, nodes_even)

    def one_group(p, carry):
        @pl.when(p < (n - ahead) // 16)
        def _():
            for i in range(16):
                block_copy(ahead + p * 16 + i).start()

        @pl.when(p < n // group - 1)
        def _():
            arrived(p * group + 2, group, p + 1).wait_recv()

        @pl.when(p == n // group - 1)
        def _():
            arrived(n - group + 2, group - 2, n // group).wait_recv()

        first = p * (group // 2)

        for t in range(group // 4):
            gather(first + 2 * t + 1, nodes_odd)
            weigh_pair(first + 2 * t, nodes_even)
            gather(jnp.minimum(first + 2 * t + 2, n // 2 - 1), nodes_even)
            weigh_pair(first + 2 * t + 1, nodes_odd)
        return carry

    lax.fori_loop(0, n // group, one_group, 0)

    arrived(1, n - 1, 0).wait_send()
    for k in range(8):
        @pl.when(exists(k))
        def _(k=k):
            halo_copy(k, 7 - k).wait_send()


def shards(particles, dest_key, cell_a, cell_b, velocity):
    owners = lax.axis_size(("gx", "gy", "gz"))
    count = particles.shape[1]
    cap = 4 * count // owners
    tile_height, tile_width = velocity.shape[1:]
    assert owners == LANES and cap == 2 * LANES and (tile_height, tile_width) == (256, 128)
    width, chunk = 256, 1024
    tops = count // width
    sizes = tuple(lax.axis_size(name) for name in ("gx", "gy", "gz"))
    in_vmem = pl.BlockSpec(memory_space=pltpu.VMEM)
    rows = 12 * BLOCK_B + 32
    binned, binned_cell = pl.pallas_call(
        functools.partial(exchange_kernel, sizes, width, chunk),
        out_shape=(jax.ShapeDtypeStruct((8, owners * cap), jnp.float32),
                   jax.ShapeDtypeStruct((owners * 2, LANES), jnp.int32)),
        in_specs=[in_vmem] * 5,
        out_specs=(in_vmem,) * 2,
        scratch_shapes=[
            pltpu.VMEM((owners, count), jnp.bfloat16),
            pltpu.VMEM((tops, owners, LANES), jnp.float32),
            pltpu.VMEM((tops * 18, chunk), jnp.bfloat16),
            pltpu.VMEM((width, chunk), jnp.bfloat16),
            pltpu.VMEM((tops * 18, width), jnp.float32),
            pltpu.VMEM((count // LANES + 3, 8, LANES), jnp.float32),
            pltpu.VMEM((count // LANES + 3, 8, LANES), jnp.float32),
            pltpu.VMEM((8, LANES), jnp.int32),
            pltpu.SMEM((8, LANES), jnp.int32),
            pltpu.VMEM((owners, 18, LANES), jnp.float32),
            pltpu.VMEM((owners, 18, LANES), jnp.float32),
            pltpu.VMEM((8, max(tile_height, tile_width)), jnp.float32),
            pltpu.VMEM((8, 8, max(tile_height, tile_width)), jnp.float32),
            pltpu.VMEM((rows, TERMS * 256), NARROW),
            pltpu.VMEM((8, LANES), jnp.float32),
            pltpu.VMEM((rows, 4 * LANES), jnp.float32),
            pltpu.VMEM((rows, 4 * LANES), jnp.float32),
            pltpu.SemaphoreType.DMA,
            pltpu.SemaphoreType.DMA((owners // 16 + 1,)),
            pltpu.SemaphoreType.DMA((8,)),
            pltpu.SemaphoreType.DMA((8,)),
            pltpu.SemaphoreType.DMA,
            pltpu.SemaphoreType.REGULAR,
        ],
        compiler_params=pltpu.CompilerParams(collective_id=0, has_side_effects=True),
    )(particles, dest_key.reshape(1, -1), cell_a.reshape(1, -1), cell_b.reshape(1, -1), velocity)
    return (binned, binned_cell.reshape(-1))


def solution(mesh):
    in_specs = (
        P(None, ("gx", "gy", "gz")),
        P(("gx", "gy", "gz")),
        P(("gx", "gy", "gz")),
        P(("gx", "gy", "gz")),
        P(None, "gx", ("gy", "gz")),
    )
    out_specs = (P(None, ("gx", "gy", "gz")), P(("gx", "gy", "gz")))
    return jax.shard_map(shards, mesh=mesh, in_specs=in_specs, out_specs=out_specs, check_vma=False)
```
